128 devices in a mesh: dev: 128 (over y, x, z, core).
Axes of the slice: x: 4, y: 4, z: 4, core: 2. Of those that a mesh axis runs over, the one named last changes fastest.
Arguments:
- prior_labels: bfloat16 [262144, 512], P('dev'), may hold values from 0.0009994507 to 1
- label_class: int32 [262144], P('dev'), may hold values from 0 to 511
- labeled: int32 [262144], P('dev'), may hold values 0 or 1
- features: bfloat16 [262144, 1024], P('dev'), may hold values from -6 to 6
- tile_cols: int32 [2048, 8], P('dev'), may hold values from 0 to 17, as said below
- tile_weights: bfloat16 [2048, 8, 128, 128], P('dev'), may hold values from 0 to 1, as said below
- halo_owner: int32 [32768, 1], P('dev'), may hold values from 0 to 127; in each aligned block of 256 rows (0 to 255, 256 to 511, ...) at most 4 rows name the same one
- halo_local: int32 [32768], P('dev'), may hold values from 0 to 2047
- batch_owner: int32 [65536, 1], P('dev'), may hold values from 0 to 127; in each aligned block of 512 rows (0 to 511, 512 to 1023, ...) at most 8 rows name the same one
- batch_local: int32 [65536], P('dev'), may hold values from 0 to 2047
- w_in: bfloat16 [4096, 1024], replicated, may hold values from -0.1875 to 0.1875
- w_out: bfloat16 [4096, 512], replicated, may hold values from -0.09375 to 0.09375
Outputs:
- propagated: bfloat16 [262144, 512], P('dev')
- row_error: float32 [65536], P('dev')
- grad_in: float32 [4096, 1024], P('dev')
- grad_out: float32 [4096, 512], P('dev')
The draws below stay inside these ranges and needn't reach their ends.
Inputs may be any that keep to these rules, and one draw needn't show every extreme that they name: `tile_cols`: in each row tile's list the first 6 entries are tiles of the device's own rows (below 16), the first of them the row tile itself; the last 2 are halo tiles (16 and above). Entries may repeat. Every halo tile of a device is listed by some row tile of that device. `tile_weights`: strictly positive. `halo_owner`: within the 256 rows of one device no owner appears more than 4 times; in some device one owner appears exactly 4 times. `batch_owner`: within the 512 rows of one device no owner appears more than 8 times; in some device one owner appears exactly 8 times.
All inputs are finite; a program needn't handle non-finite values. No bound on the sum of `labeled` on one device may be relied on, other than what follows from the above.
Results may differ from the reference program's by a relative error of at most 0.0017.
Values may be sent and summed in bfloat16 or wider, within the bound.
No kernel may reach another device: no remote copies, remote signals or barrier semaphores. Data moves between devices by JAX's collectives and lax.ppermute only.
A program may use at most 128 MiB of HBM per device.

```python
import math
import jax
import jax.numpy as jnp
import numpy as np
from jax import lax

TILE = 128
CLASSES = 512
FEAT = 1024
HID = 4096
TPR_LOCAL = 6
TPR_HALO = 2
NODE_DEV = 2048
HALO_DEV = 256
BATCH_DEV = 512
TPR = 8
CAPR = 4
CAPB = 8
NODES = 262144
HALO = 32768
BATCH = 65536
N_DEV = 128


def draw_tile_cols(key, part):
    row_tiles = NODES // TILE
    own_count = NODE_DEV // TILE
    halo_count = HALO_DEV // TILE
    first_key, second_key = jax.random.split(jax.random.fold_in(key, 17))
    itself = jnp.arange(row_tiles, dtype=jnp.int32) % own_count
    nearby = jax.random.randint(first_key, (row_tiles, TPR_LOCAL - 1), 0, own_count, dtype=jnp.int32)
    covering = itself % halo_count + own_count
    remote = jax.random.randint(second_key, (row_tiles, TPR_HALO - 1), 0, halo_count, dtype=jnp.int32) + own_count
    return jnp.concatenate([itself[:, None], nearby, covering[:, None], remote], axis=1)


def draw_tile_weights(key, part):
    normal = jnp.clip(jax.random.normal(jax.random.fold_in(key, 29), (NODES // TILE, TPR, TILE, TILE), dtype=jnp.float32), -3.0, 3.0)
    spread = 2.0
    return jnp.exp(spread * (normal - 3.0)).astype(jnp.bfloat16)


def plant(entries, rng, low, largest):
    spot = [jax.random.randint(jax.random.fold_in(rng, axis), (), 0, length) for axis, length in enumerate(entries.shape)]
    longest = entries.shape.index(max(entries.shape))
    neighbour = spot[:longest] + [(spot[longest] + 1) % entries.shape[longest]] + spot[longest + 1:]
    return entries.at[tuple(spot)].set(low).at[tuple(neighbour)].set(largest)


def level_of(own_key, dims, pieces, least, high):
    gain = 1.0
    for dim, blocks in pieces:
        heights = jax.random.uniform(jax.random.fold_in(jax.random.fold_in(own_key, 6), dim), (blocks,), jnp.float32, least / len(pieces), high / len(pieces))
        gain = gain * jnp.repeat(jnp.exp(heights), dims[dim] // blocks).reshape((-1,) + (1,) * (len(dims) - 1 - dim))
    return gain


def assign_block(rng, own, number, rows, count, top, limit, slope):
    ranking = jax.random.permutation(rng, count)
    packed, usual = load_shares(count, rows * top, limit, slope, True), load_shares(count, rows * top, limit, slope, False)
    places = jnp.arange(count)

    def named(sizes, rotation):
        used = int((sizes > 0).sum())
        fixed = max(1, used // 4)
        moved = fixed + (places - fixed + rotation * (used - fixed)) % max(1, count - fixed)
        return jnp.zeros((count,), jnp.int32).at[ranking[jnp.where(places < fixed, places, moved)]].set(jnp.asarray(sizes, jnp.int32))

    sizes = jnp.where(number % 4 == 0, named(packed, number // 4), named(usual, number - number // 4 - 1))
    mixed = jax.random.permutation(jax.random.fold_in(own, 3), count)
    source_of, taker = mixed[0:count // 2 * 2:2], mixed[1:count // 2 * 2:2]
    slack = jnp.minimum(sizes[source_of] - 1, limit - sizes[taker]) // 2
    slack = jnp.where((source_of == ranking[0]) | (taker == ranking[0]) | (sizes[taker] == 0), 0, jnp.maximum(slack, 0))
    moved = jax.random.randint(jax.random.fold_in(own, 4), (count // 2,), 0, 1 << 20) % (slack + 1)
    sizes = sizes.at[source_of].add(-moved).at[taker].add(moved)
    labels = jnp.searchsorted(jnp.cumsum(sizes), jnp.arange(rows * top), side="right").astype(jnp.int32)
    table = labels.reshape(top, rows).T
    table = table[jax.random.permutation(jax.random.fold_in(own, 1), rows)]
    rotation = jax.random.randint(jax.random.fold_in(own, 2), (rows, 1), 0, top)
    return jnp.take_along_axis(table, (jnp.arange(top)[None, :] + rotation) % top, axis=1)


def load_shares(number_of, total, limit, skew, full):
    weights = [(1 << 20) // math.isqrt(standing ** skew) + 1 for standing in range(1, number_of + 1)]
    largest = limit if full else min(limit, max(-(-total // number_of), total * weights[0] // sum(weights)))
    least = 1 if total - largest >= number_of - 1 else 0
    holding, spare = [largest] + [least] * (number_of - 1), total - largest - least * (number_of - 1)
    while spare > 0:
        movable = [i for i in range(1, number_of) if holding[i] < largest] or [i for i in range(1, number_of) if holding[i] < limit]
        whole, left = sum([weights[i] for i in movable]), spare
        for i in movable:
            more = min(limit - holding[i], max(1, left * weights[i] // whole), spare)
            holding[i] = holding[i] + more
            spare = spare - more
    return np.array(holding)


def noise(rng, shape, width, limit, cuts=(), held_as=jnp.bfloat16):
    level = level_of(rng, shape, cuts, -0.22, 0.18) if cuts else 1.0
    drawn = jax.random.normal(rng, shape, jnp.float32) * width * level
    return jnp.minimum(jnp.maximum(drawn, -limit), limit).astype(held_as)


def setup_inputs(seed: int = 0) -> dict:
    key_of = jax.random.split(jax.random.key(seed), 13)
    prior_labels = jnp.clip(jnp.exp(math.log(1.0) - 6.9083047 * jax.random.uniform(key_of[0], (NODES, CLASSES), jnp.float32) ** level_of(key_of[0], (NODES, CLASSES), ((0, 128),), -0.2, 0.2)), 0.0009994507, 1.0).astype(jnp.bfloat16)
    label_class = plant(jax.random.randint(key_of[1], (NODES,), 0, CLASSES), jax.random.fold_in(key_of[1], 1), 0, CLASSES - 1).astype(jnp.int32)
    labeled = plant((jax.random.randint(key_of[2], (NODES,), 0, 4) < 1).astype(jnp.int32), jax.random.fold_in(key_of[2], 1), 0, 1)
    features = noise(key_of[3], (NODES, FEAT), 1.0, 6.0, ((0, 128),))
    tile_cols = draw_tile_cols(jax.random.fold_in(key_of[12], 71), 0)
    tile_weights = draw_tile_weights(jax.random.fold_in(key_of[12], 71), 0)
    halo_owner_keys = jax.random.split(jax.random.fold_in(key_of[6], 1), HALO // HALO_DEV)
    halo_owner_turns = jax.random.permutation(jax.random.fold_in(key_of[6], 3), HALO // HALO_DEV)
    halo_owner = jax.vmap(lambda own, number: assign_block(jax.random.fold_in(key_of[6], 2), own, number, HALO_DEV, N_DEV, 1, CAPR, 1))(halo_owner_keys, halo_owner_turns).reshape((HALO, 1))
    halo_local = plant(jax.random.randint(key_of[7], (HALO,), 0, NODE_DEV), jax.random.fold_in(key_of[7], 1), 0, NODE_DEV - 1).astype(jnp.int32)
    batch_owner_keys = jax.random.split(jax.random.fold_in(key_of[8], 1), BATCH // BATCH_DEV)
    batch_owner_turns = jax.random.permutation(jax.random.fold_in(key_of[8], 3), BATCH // BATCH_DEV)
    batch_owner = jax.vmap(lambda own, number: assign_block(jax.random.fold_in(key_of[8], 2), own, number, BATCH_DEV, N_DEV, 1, CAPB, 1))(batch_owner_keys, batch_owner_turns).reshape((BATCH, 1))
    batch_local = plant(jax.random.randint(key_of[9], (BATCH,), 0, NODE_DEV), jax.random.fold_in(key_of[9], 1), 0, NODE_DEV - 1).astype(jnp.int32)
    w_in = noise(key_of[10], (HID, FEAT), FEAT ** -0.5, 0.1875)
    w_out = noise(key_of[11], (HID, CLASSES), HID ** -0.5, 0.09375)
    return {"prior_labels": prior_labels, "label_class": label_class, "labeled": labeled, "features": features, "tile_cols": tile_cols, "tile_weights": tile_weights, "halo_owner": halo_owner, "halo_local": halo_local, "batch_owner": batch_owner, "batch_local": batch_local, "w_in": w_in, "w_out": w_out}


def reference(prior_labels, label_class, labeled, features, tile_cols, tile_weights, halo_owner, halo_local, batch_owner, batch_local, w_in, w_out):
    devices = N_DEV
    own_tiles = NODE_DEV // TILE
    halo_tiles = HALO_DEV // TILE
    halo_node = (halo_owner[:, 0] * NODE_DEV + halo_local).astype(jnp.int32)
    halo_labels = prior_labels[halo_node]
    table = jnp.concatenate([prior_labels.reshape(devices, own_tiles, TILE, CLASSES), halo_labels.reshape(devices, halo_tiles, TILE, CLASSES)], axis=1)
    columns = tile_cols.reshape(devices, own_tiles, TPR)
    weights = tile_weights.reshape(devices, own_tiles, TPR, TILE, TILE)
    given_class = label_class.reshape(devices, NODE_DEV)
    marked = labeled.reshape(devices, NODE_DEV)

    def one_device(inputs):
        block_table, block_cols, block_weights, block_class, block_mark = inputs
        blocks = block_table[block_cols].astype(jnp.float32)
        wide_weights = block_weights.astype(jnp.float32)
        spread = jnp.einsum('rkij,rkjc->ric', wide_weights, blocks, precision=lax.Precision.HIGHEST)
        degree = lax.optimization_barrier(jnp.sum(wide_weights, axis=(1, 3)))
        seeds = ((block_class[:, None] == jnp.arange(CLASSES, dtype=jnp.int32)[None, :]) & (block_mark[:, None] == 1)).astype(jnp.float32)
        mixed = 0.8 * (spread / degree[:, :, None]).reshape(NODE_DEV, CLASSES) + 0.2 * seeds
        return mixed.astype(jnp.bfloat16)
    propagated = lax.map(one_device, (table, columns, weights, given_class, marked)).reshape(NODES, CLASSES)
    batch_node = (batch_owner[:, 0] * NODE_DEV + batch_local).astype(jnp.int32)
    batch_x = features[batch_node]
    batch_z = propagated[batch_node]
    log_z = jnp.log(batch_z.astype(jnp.float32))
    target = log_z - lax.optimization_barrier(jnp.mean(log_z, axis=1, keepdims=True))
    hidden = jnp.tanh(jnp.dot(batch_x, w_in.T, preferred_element_type=jnp.float32)).astype(jnp.bfloat16)
    logits = jnp.dot(hidden, w_out, preferred_element_type=jnp.float32)
    differ = logits - target
    row_error = 0.5 * lax.optimization_barrier(jnp.mean(differ * differ, axis=1))
    residue = (differ / math.sqrt(BATCH)).astype(jnp.bfloat16)
    grad_out = jnp.dot(hidden.T, residue, preferred_element_type=jnp.float32)
    hidden_wide = hidden.astype(jnp.float32)
    back = (jnp.dot(residue, w_out.T, preferred_element_type=jnp.float32) * (1.0 - hidden_wide * hidden_wide)).astype(jnp.bfloat16)
    grad_in = jnp.dot(back.T, batch_x, preferred_element_type=jnp.float32)
    return (propagated, row_error, grad_in, grad_out)
```

```python
import jax
import jax.numpy as jnp
from jax import lax
from jax.experimental import pallas as pl
from jax.experimental.pallas import tpu as pltpu
from jax.sharding import Mesh
from jax.sharding import PartitionSpec as P


DEV = "dev"
BF = jnp.bfloat16
F32 = jnp.float32
LANES = 128
HALO_SLOTS = 4
BATCH_SLOTS = 8
UNITS = 32
HBLK = 512


def params(mib=48, **more):
    return pltpu.CompilerParams(vmem_limit_bytes=mib * 2**20, **more)


def dot(left, right, dims):
    return lax.dot_general(left, right, ((dims[:1], dims[1:]), ((), ())), preferred_element_type=F32)


def ranks_of(owner_ref, blocks):
    below = lax.broadcasted_iota(jnp.int32, (LANES, LANES), 0)
    along = lax.broadcasted_iota(jnp.int32, (LANES, LANES), 1)
    rows = [owner_ref[b : b + 1, :] for b in range(blocks)]
    cols = [jnp.broadcast_to(row, (LANES, LANES)).T for row in rows]
    ranks = []
    for i in range(blocks):
        earlier = jnp.zeros((LANES, LANES), F32)
        for j in range(i + 1):
            same = cols[j] == rows[i]
            if j == i:
                same = same & (below < along)
            earlier = earlier + same.astype(F32)
        ranks.append(jnp.sum(earlier, axis=0, keepdims=True).astype(jnp.int32))
    return rows, ranks


def request_kernel(ho, hl, bo, bl, table, hslot, brank):
    device = lax.broadcasted_iota(jnp.int32, (LANES, LANES), 0)
    lane = lax.broadcasted_iota(jnp.int32, (LANES, LANES), 1)
    out = jnp.zeros((LANES, LANES), F32)
    at = 0
    for owner, local, count in ((ho, hl, HALO_SLOTS), (bo, bl, BATCH_SLOTS)):
        blocks = owner.shape[0]
        rows, ranks = ranks_of(owner, blocks)
        for s in range(count):
            total = jnp.zeros((LANES, LANES), F32)
            for i in range(blocks):
                hit = (device == rows[i]) & (ranks[i] == s)
                named = (local[i : i + 1, :] + 1).astype(F32)
                total = total + jnp.where(hit, jnp.broadcast_to(named, (LANES, LANES)), 0.0)
            out = jnp.where(lane == at, jnp.sum(total, axis=1, keepdims=True), out)
            at += 1
        for i in range(blocks):
            if owner is ho:
                hslot[i : i + 1, :] = rows[i] * HALO_SLOTS + ranks[i]
            else:
                brank[i : i + 1, :] = ranks[i]
    table[...] = out.astype(jnp.int32) - 1


def returned_kernel(errors, bo, brank, out):
    device = lax.broadcasted_iota(jnp.int32, (LANES, LANES), 0)
    for i in range(bo.shape[0]):
        total = jnp.zeros((LANES, LANES), F32)
        for s in range(BATCH_SLOTS):
            hit = (device == bo[i : i + 1, :]) & (brank[i : i + 1, :] == s)
            total = total + jnp.where(hit, errors[:, s : s + 1], 0.0)
        out[i : i + 1, :] = jnp.sum(total, axis=0, keepdims=True)


def reorder_kernel(place, w_in, w_out, w_in_to, w_out_to, sem_a, sem_b):
    core = place[3]

    def chunk(q, _):
        half = q // 64
        holder = jnp.where(half == 1, core, 1 - core)
        turn = 1 - holder
        a = ((q // 16) % 4 + turn) % 4
        b = ((q // 4) % 4 + turn) % 4
        c = (q % 4 + turn) % 4
        source = ((a * 4 + b) * 4 + c) * 2 + holder
        pltpu.make_async_copy(w_in.at[source], w_in_to.at[q], sem_a).start()
        pltpu.make_async_copy(w_out.at[source], w_out_to.at[q], sem_b).start()
        return 0

    lax.fori_loop(0, 128, chunk, 0)
    pltpu.make_async_copy(w_in, w_in_to, sem_a).wait()
    pltpu.make_async_copy(w_out, w_out_to, sem_b).wait()


def pick_rows(table, first, count, nodes, onehot):
    node = lax.broadcasted_iota(jnp.int32, (LANES, nodes), 1)
    for s in range(count):
        wanted = table[:, first + s : first + s + 1]
        onehot[s * LANES : (s + 1) * LANES, :] = (node == wanted).astype(F32).astype(BF)


def forward_kernel(table, features, w_in, w_out, x, hidden, logits, onehot, acc):
    step = pl.program_id(0)

    @pl.when(step == 0)
    def _():
        pick_rows(table, HALO_SLOTS, BATCH_SLOTS, features.shape[0], onehot)
        x[...] = dot(onehot[...], features[...], (1, 0)).astype(BF)
        acc[...] = jnp.zeros(acc.shape, F32)

    h = jnp.tanh(dot(w_in[...], x[...], (1, 1))).astype(BF)
    hidden[...] = h
    acc[...] += dot(w_out[...], h, (0, 0))

    @pl.when(step == pl.num_programs(0) - 1)
    def _():
        logits[...] = acc[...].T


def spread_kernel(cols, weights, prior, halo, hslot, given, table, logits, prop, residue, errors, halo_tab, prop_all, onehot):
    step = pl.program_id(0)
    per = weights.shape[0]
    classes = prior.shape[1]

    @pl.when(step == 0)
    def _():
        slots = halo.shape[0]
        slot = lax.broadcasted_iota(jnp.int32, (slots, LANES), 0)
        for b in range(2):
            pick = (slot == hslot[b : b + 1, :]).astype(F32).astype(BF)
            halo_tab[b * LANES : (b + 1) * LANES, :] = dot(pick, halo[...], (0, 0)).astype(BF)

    for t in range(per):
        r = step * per + t
        acc = jnp.zeros((LANES, classes), F32)
        wide = jnp.zeros((LANES, LANES), F32)
        for m in range(4):
            pair = []
            for k in (2 * m, 2 * m + 1):
                wide = wide + weights[t, k].astype(F32)
                c = cols[r, k]
                if k < 6:
                    pair.append(prior[pl.ds(pl.multiple_of(c * LANES, LANES), LANES), :])
                else:
                    pair.append(halo_tab[pl.ds(pl.multiple_of((c - 16) * LANES, LANES), LANES), :])
            left = jnp.concatenate([weights[t, 2 * m], weights[t, 2 * m + 1]], axis=1)
            acc = acc + dot(left, jnp.concatenate(pair, axis=0), (1, 0))
        degree = jnp.sum(wide, axis=1, keepdims=True)
        mark = jnp.broadcast_to(given[pl.ds(r, 1), :], (LANES, LANES)).T
        lane = lax.broadcasted_iota(jnp.int32, (LANES, LANES), 1)
        seeds = jnp.concatenate([(mark == lane + g * LANES).astype(F32) for g in range(classes // LANES)], axis=1)
        mixed = (0.8 * (acc / degree) + 0.2 * seeds).astype(BF)
        prop[t * LANES : (t + 1) * LANES, :] = mixed
        prop_all[pl.ds(pl.multiple_of(r * LANES, LANES), LANES), :] = mixed

    @pl.when(step == pl.num_programs(0) - 1)
    def _():
        pick_rows(table, HALO_SLOTS, BATCH_SLOTS, prop_all.shape[0], onehot)
        lane = lax.broadcasted_iota(jnp.int32, (LANES, LANES), 1)
        out = jnp.zeros((LANES, LANES), F32)
        for s in range(BATCH_SLOTS):
            at = slice(s * LANES, (s + 1) * LANES)
            log_z = jnp.log(dot(onehot[at, :], prop_all[...], (1, 0)))
            target = log_z - jnp.mean(log_z, axis=1, keepdims=True)
            valid = table[:, HALO_SLOTS + s : HALO_SLOTS + s + 1] >= 0
            differ = jnp.where(valid, logits[at, :] - target, 0.0)
            out = jnp.where(lane == s, 0.5 * jnp.mean(differ * differ, axis=1, keepdims=True), out)
            residue[at, :] = (differ * (1.0 / 256.0)).astype(BF)
        errors[...] = out


def out_send_kernel(hidden, residue, grad):
    grad[...] = dot(hidden[...], residue[...], (1, 0)).astype(BF)


def back_of(w_out, hidden, residue):
    wide = hidden[...].astype(F32)
    return (dot(w_out[...], residue[...], (1, 1)) * (1.0 - wide * wide)).astype(BF)


def in_send_kernel(w_out, hidden, residue, x, grad):
    grad[...] = dot(back_of(w_out, hidden, residue), x[...], (1, 0)).astype(BF)


def out_own_kernel(place, hidden, residue, arrived, send, keep):
    total = (dot(hidden[...], residue[...], (1, 0)) + arrived[...].astype(F32)).astype(BF)
    step = pl.program_id(0)

    @pl.when(step < 2)
    def _():
        send[...] = total

    @pl.when(step >= 2)
    def _():
        keep[...] = total


def in_own_kernel(place, w_out, hidden, residue, x, arrived, send_b, keep_b, send_c, keep_c):
    total = (dot(back_of(w_out, hidden, residue), x[...], (1, 0)) + arrived[...].astype(F32)).astype(BF)
    left = total[:, :512].reshape(2, 256, 512)
    right = total[:, 512:].reshape(4, 2, 64, 512)

    for half in range(2):

        @pl.when(place[1] == half)
        def _():
            keep_b[0] = left[half]
            send_b[0] = left[1 - half]

        @pl.when(place[2] == half)
        def _():
            keep_c[0] = right[:, half]
            send_c[0] = right[:, 1 - half]


def pairing(level, dims):
    flip = 3 if level == 1 else 1
    pairs = []
    for source in range(128):
        core = source % 2
        spot = [source // 32, (source // 8) % 4, (source // 2) % 4]
        for d in dims:
            shifted = (spot[d] - (1 - core)) % 4
            spot[d] = ((shifted ^ flip) + (1 - core)) % 4
        pairs.append((source, ((spot[0] * 4 + spot[1]) * 4 + spot[2]) * 2 + core))
    return pairs


def exchange(x, level, dims):
    return lax.ppermute(x, DEV, pairing(level, dims))


def deal_kernel(bits, k0, r0, k1, r1, k2, r2, own, *sends):
    for m in range(8):
        a = bits[0] ^ (m >> 2)
        b = bits[1] ^ ((m >> 1) & 1)
        c = bits[2] ^ (m & 1)
        for j, (k, r) in enumerate(((k0, r0), (k1, r1), (k2, r2))):
            piece = k[a, b, c].astype(F32) + r[a, b, c].astype(F32)
            if m == 0:
                own[:, j * 512 : (j + 1) * 512] = piece
            else:
                sends[m - 1][:, j * 512 : (j + 1) * 512] = piece.astype(BF)


def summed_over_chips(sends, keeps, halves, bits):
    shapes = ((2, 4, 4), (4, 2, 4), (4, 4, 2))
    keep = [k.reshape(*s, UNITS, 512) for k, s in zip(keeps, shapes)]
    got = [exchange(s, 1, (j,)).reshape(keep[j].shape) for j, s in enumerate(sends)]
    for step in (1, 2):
        dims = [(j + step) % 3 for j in range(3)]
        sent = []
        for j, d in enumerate(dims):
            part = lambda v, h: lax.dynamic_slice_in_dim(v, 2 * h, 2, d)
            other = 1 - halves[d]
            out = (part(keep[j], other).astype(F32) + part(got[j], other).astype(F32)).astype(BF)
            sent.append(exchange(out, 1, (d,)))
            keep[j] = (part(keep[j], halves[d]).astype(F32) + part(got[j], halves[d]).astype(F32)).astype(F32 if step == 2 else BF)
        got = sent
    piece = jax.ShapeDtypeStruct((UNITS, 1536), BF)
    own, *pieces = pl.pallas_call(
        deal_kernel,
        in_specs=[pl.BlockSpec(memory_space=pltpu.SMEM)] + [pl.BlockSpec(memory_space=pltpu.VMEM)] * 6,
        out_shape=[jax.ShapeDtypeStruct((UNITS, 1536), F32)] + [piece] * 7,
        compiler_params=params(),
        name="deal",
    )(bits, keep[0], got[0], keep[1], got[1], keep[2], got[2])
    total = own
    for m in range(1, 8):
        dims = [d for d in range(3) if (m >> (2 - d)) & 1]
        total = total + exchange(pieces[m - 1], 2, dims).astype(F32)
    return total


def on_device(prior, label_class, labeled, features, tile_cols, tile_weights, halo_owner, halo_local, batch_owner, batch_local, w_in, w_out):
    nodes, classes = prior.shape
    feat = features.shape[1]
    hid = w_in.shape[0]
    halo_count = halo_local.shape[0]
    batch = batch_local.shape[0]
    rows = BATCH_SLOTS * LANES
    me = lax.axis_index(DEV)
    core = me % 2
    turn = 1 - core
    spots = [(s + 4 - turn) % 4 for s in (me // 32, (me // 8) % 4, (me // 2) % 4)]
    halves = [s // 2 for s in spots]
    place = jnp.stack([*halves, core]).astype(jnp.int32)
    bits = jnp.stack([s % 2 for s in spots]).astype(jnp.int32)
    vmem = pl.BlockSpec(memory_space=pltpu.VMEM)
    smem = pl.BlockSpec(memory_space=pltpu.SMEM)
    hbm = pl.BlockSpec(memory_space=pl.ANY)
    i32 = jnp.int32

    bo = batch_owner.reshape(batch // LANES, LANES)
    table, hslot, brank = pl.pallas_call(
        request_kernel,
        in_specs=[vmem] * 4,
        out_shape=[
            jax.ShapeDtypeStruct((LANES, LANES), i32),
            jax.ShapeDtypeStruct((halo_count // LANES, LANES), i32),
            jax.ShapeDtypeStruct((batch // LANES, LANES), i32),
        ],
        name="request",
    )(
        halo_owner.reshape(halo_count // LANES, LANES),
        halo_local.reshape(halo_count // LANES, LANES),
        bo,
        batch_local.reshape(batch // LANES, LANES),
    )
    asked = lax.all_to_all(table, DEV, 0, 0, tiled=True)

    w_in_o, w_out_o = pl.pallas_call(
        reorder_kernel,
        in_specs=[smem, hbm, hbm],
        out_specs=[hbm, hbm],
        out_shape=[jax.ShapeDtypeStruct((128, UNITS, feat), BF), jax.ShapeDtypeStruct((128, UNITS, classes), BF)],
        scratch_shapes=[pltpu.SemaphoreType.DMA, pltpu.SemaphoreType.DMA],
        name="reorder",
    )(place, w_in.reshape(128, UNITS, feat), w_out.reshape(128, UNITS, classes))
    w_in_o = w_in_o.reshape(hid, feat)
    w_out_o = w_out_o.reshape(hid, classes)

    served = prior[jnp.maximum(asked[:, :HALO_SLOTS], 0)]
    halo = lax.all_to_all(served, DEV, 0, 0, tiled=True).reshape(LANES * HALO_SLOTS, classes)

    def whole(shape):
        return pl.BlockSpec(shape, lambda i, *_: (0,) * len(shape))

    def once(shape):
        return pl.BlockSpec(shape, lambda i, *_: (0,) * len(shape), pipeline_mode=pl.Buffered(1))

    def rows_at(offset, width):
        return pl.BlockSpec((HBLK, width), lambda i, *_: (i + offset, 0))

    x, hidden, logits = pl.pallas_call(
        forward_kernel,
        grid=(hid // HBLK,),
        in_specs=[once((LANES, LANES)), once((nodes, feat)), rows_at(0, feat), rows_at(0, classes)],
        out_specs=[whole((rows, feat)), rows_at(0, rows), whole((rows, classes))],
        out_shape=[
            jax.ShapeDtypeStruct((rows, feat), BF),
            jax.ShapeDtypeStruct((hid, rows), BF),
            jax.ShapeDtypeStruct((rows, classes), F32),
        ],
        scratch_shapes=[pltpu.VMEM((rows, nodes), BF), pltpu.VMEM((classes, rows), F32)],
        compiler_params=params(),
        name="forward",
    )(asked, features, w_in_o, w_out_o)

    row_tiles = tile_weights.shape[0]
    per = 2
    given = jnp.where(labeled == 1, label_class, -1).reshape(row_tiles, LANES)
    prop, residue, errors = pl.pallas_call(
        spread_kernel,
        grid=(row_tiles // per,),
        in_specs=[
            smem,
            pl.BlockSpec((per, 8, LANES, LANES), lambda i: (i, 0, 0, 0)),
            once((nodes, classes)),
            once((LANES * HALO_SLOTS, classes)),
            once((halo_count // LANES, LANES)),
            once((row_tiles, LANES)),
            once((LANES, LANES)),
            once((rows, classes)),
        ],
        out_specs=[
            pl.BlockSpec((per * LANES, classes), lambda i: (i, 0)),
            whole((rows, classes)),
            whole((LANES, LANES)),
        ],
        out_shape=[
            jax.ShapeDtypeStruct((nodes, classes), BF),
            jax.ShapeDtypeStruct((rows, classes), BF),
            jax.ShapeDtypeStruct((LANES, LANES), F32),
        ],
        scratch_shapes=[
            pltpu.VMEM((halo_count, classes), BF),
            pltpu.VMEM((nodes, classes), BF),
            pltpu.VMEM((rows, nodes), BF),
        ],
        compiler_params=params(),
        name="spread",
    )(tile_cols, tile_weights, prior, halo, hslot, given, asked, logits)

    back_errors = lax.all_to_all(errors, DEV, 0, 0, tiled=True)
    row_error = pl.pallas_call(
        returned_kernel,
        in_specs=[vmem] * 3,
        out_shape=jax.ShapeDtypeStruct((batch // LANES, LANES), F32),
        name="returned",
    )(back_errors, bo, brank).reshape(batch)

    steps = hid // 2 // HBLK
    partner = [(d, d ^ 1) for d in range(128)]
    half_out = jax.ShapeDtypeStruct((hid // 2, classes), BF)
    out_peer = pl.pallas_call(
        out_send_kernel,
        grid=(steps,),
        in_specs=[rows_at(0, rows), once((rows, classes))],
        out_specs=rows_at(0, classes),
        out_shape=half_out,
        compiler_params=params(),
        name="out_peer",
    )(hidden, residue)
    out_arrived = lax.ppermute(out_peer, DEV, partner)
    in_peer = pl.pallas_call(
        in_send_kernel,
        grid=(steps,),
        in_specs=[rows_at(0, classes), rows_at(0, rows), once((rows, classes)), once((rows, feat))],
        out_specs=rows_at(0, feat),
        out_shape=jax.ShapeDtypeStruct((hid // 2, feat), BF),
        compiler_params=params(),
        name="in_peer",
    )(w_out_o, hidden, residue, x)
    in_arrived = lax.ppermute(in_peer, DEV, partner)

    def block(i, p):
        return (i + 2 * (1 - p[0])) % 4

    quarter = jax.ShapeDtypeStruct((hid // 4, classes), BF)
    out_send, out_keep = pl.pallas_call(
        out_own_kernel,
        grid_spec=pltpu.PrefetchScalarGridSpec(
            num_scalar_prefetch=1,
            grid=(steps,),
            in_specs=[
                pl.BlockSpec((HBLK, rows), lambda i, p: (block(i, p) + steps, 0)),
                once((rows, classes)),
                pl.BlockSpec((HBLK, classes), lambda i, p: (block(i, p), 0)),
            ],
            out_specs=[
                pl.BlockSpec((HBLK, classes), lambda i, p: (jnp.minimum(i, 1), 0)),
                pl.BlockSpec((HBLK, classes), lambda i, p: (jnp.maximum(i - 2, 0), 0)),
            ],
        ),
        out_shape=[quarter, quarter],
        compiler_params=params(),
        name="out_own",
    )(place, hidden, residue, out_arrived)
    b_spec = pl.BlockSpec((1, 256, 512), lambda i, p: (i, 0, 0))
    c_spec = pl.BlockSpec((1, 4, 64, 512), lambda i, p: (i, 0, 0, 0))
    b_shape = jax.ShapeDtypeStruct((4, 256, 512), BF)
    c_shape = jax.ShapeDtypeStruct((4, 4, 64, 512), BF)
    b_send, b_keep, c_send, c_keep = pl.pallas_call(
        in_own_kernel,
        grid_spec=pltpu.PrefetchScalarGridSpec(
            num_scalar_prefetch=1,
            grid=(steps,),
            in_specs=[
                rows_at(steps, classes),
                rows_at(steps, rows),
                once((rows, classes)),
                once((rows, feat)),
                rows_at(0, feat),
            ],
            out_specs=[b_spec, b_spec, c_spec, c_spec],
        ),
        out_shape=[b_shape, b_shape, c_shape, c_shape],
        compiler_params=params(),
        name="in_own",
    )(place, w_out_o, hidden, residue, x, in_arrived)

    total = summed_over_chips((out_send, b_send, c_send), (out_keep, b_keep, c_keep), halves, bits)
    return prop, row_error, total[:, 512:], total[:, :512]


def solution(mesh):
    split = Mesh(mesh.devices.reshape(128), (DEV,))
    in_specs = (
        P(DEV, None),
        P(DEV),
        P(DEV),
        P(DEV, None),
        P(DEV, None),
        P(DEV, None, None, None),
        P(DEV, None),
        P(DEV),
        P(DEV, None),
        P(DEV),
        P(),
        P(),
    )
    out_specs = (P(DEV, None), P(DEV), P(DEV, None), P(DEV, None))
    return jax.shard_map(on_device, mesh=split, in_specs=in_specs, out_specs=out_specs, check_vma=False)
```

```python
import jax
import jax.numpy as jnp
from jax import lax
from jax.experimental import pallas as pl
from jax.experimental.pallas import tpu as pltpu
from jax.sharding import Mesh
from jax.sharding import PartitionSpec as P


DEV = "dev"
BF = jnp.bfloat16
F32 = jnp.float32
LANES = 128
HALO_SLOTS = 4
BATCH_SLOTS = 8
UNITS = 32
HBLK = 512


def params(mib=48, **more):
    return pltpu.CompilerParams(vmem_limit_bytes=mib * 2**20, **more)


def dot(left, right, dims):
    return lax.dot_general(left, right, ((dims[:1], dims[1:]), ((), ())), preferred_element_type=F32)


def ranks_of(owner_ref, blocks):
    below = lax.broadcasted_iota(jnp.int32, (LANES, LANES), 0)
    along = lax.broadcasted_iota(jnp.int32, (LANES, LANES), 1)
    rows = [owner_ref[b : b + 1, :] for b in range(blocks)]
    cols = [jnp.broadcast_to(row, (LANES, LANES)).T for row in rows]
    ranks = []
    for i in range(blocks):
        earlier = jnp.zeros((LANES, LANES), F32)
        for j in range(i + 1):
            same = cols[j] == rows[i]
            if j == i:
                same = same & (below < along)
            earlier = earlier + same.astype(F32)
        ranks.append(jnp.sum(earlier, axis=0, keepdims=True).astype(jnp.int32))
    return rows, ranks


def request_kernel(ho, hl, bo, bl, table, hslot, brank):
    device = lax.broadcasted_iota(jnp.int32, (LANES, LANES), 0)
    lane = lax.broadcasted_iota(jnp.int32, (LANES, LANES), 1)
    out = jnp.zeros((LANES, LANES), F32)
    at = 0
    for owner, local, count in ((ho, hl, HALO_SLOTS), (bo, bl, BATCH_SLOTS)):
        blocks = owner.shape[0]
        rows, ranks = ranks_of(owner, blocks)
        for s in range(count):
            total = jnp.zeros((LANES, LANES), F32)
            for i in range(blocks):
                hit = (device == rows[i]) & (ranks[i] == s)
                named = (local[i : i + 1, :] + 1).astype(F32)
                total = total + jnp.where(hit, jnp.broadcast_to(named, (LANES, LANES)), 0.0)
            out = jnp.where(lane == at, jnp.sum(total, axis=1, keepdims=True), out)
            at += 1
        for i in range(blocks):
            if owner is ho:
                hslot[i : i + 1, :] = rows[i] * HALO_SLOTS + ranks[i]
            else:
                brank[i : i + 1, :] = ranks[i]
    table[...] = out.astype(jnp.int32) - 1


def returned_kernel(errors, bo, brank, out):
    device = lax.broadcasted_iota(jnp.int32, (LANES, LANES), 0)
    for i in range(bo.shape[0]):
        total = jnp.zeros((LANES, LANES), F32)
        for s in range(BATCH_SLOTS):
            hit = (device == bo[i : i + 1, :]) & (brank[i : i + 1, :] == s)
            total = total + jnp.where(hit, errors[:, s : s + 1], 0.0)
        out[i : i + 1, :] = jnp.sum(total, axis=0, keepdims=True)


def pick_rows(table, first, count, nodes, onehot):
    node = lax.broadcasted_iota(jnp.int32, (LANES, nodes), 1)
    for s in range(count):
        wanted = table[:, first + s : first + s + 1]
        onehot[s * LANES : (s + 1) * LANES, :] = (node == wanted).astype(F32).astype(BF)


def forward_kernel(place, table, features, w_in, w_out, x, hidden, logits, w_out_to, onehot, acc, in_buf, out_buf, in_sem, out_sem):
    step = pl.program_id(0)
    steps = pl.num_programs(0)
    chunks = HBLK // UNITS
    core = place[3]

    def fetch(block, slot):
        half = block // 4
        holder = jnp.where(half == 1, core, 1 - core)
        turn = 1 - holder
        a = (block % 4 + turn) % 4
        for n in range(chunks):
            b = (n // 4 + turn) % 4
            c = (n % 4 + turn) % 4
            source = ((a * 4 + b) * 4 + c) * 2 + holder
            pltpu.make_async_copy(w_in.at[source], in_buf.at[slot, n], in_sem.at[slot]).start()
            pltpu.make_async_copy(w_out.at[source], out_buf.at[slot, n], out_sem.at[slot]).start()

    @pl.when(step == 0)
    def _():
        fetch(0, 0)
        pick_rows(table, HALO_SLOTS, BATCH_SLOTS, features.shape[0], onehot)
        x[...] = dot(onehot[...], features[...], (1, 0)).astype(BF)
        acc[...] = jnp.zeros(acc.shape, F32)

    slot = step % 2

    @pl.when(step + 1 < steps)
    def _():
        fetch(step + 1, 1 - slot)

    pltpu.make_async_copy(w_in.at[pl.ds(0, chunks)], in_buf.at[slot], in_sem.at[slot]).wait()
    pltpu.make_async_copy(w_out.at[pl.ds(0, chunks)], out_buf.at[slot], out_sem.at[slot]).wait()
    w_out_here = out_buf[slot].reshape(HBLK, out_buf.shape[3])
    w_out_to[...] = w_out_here
    h = jnp.tanh(dot(in_buf[slot].reshape(HBLK, in_buf.shape[3]), x[...], (1, 1))).astype(BF)
    hidden[...] = h
    acc[...] += dot(w_out_here, h, (0, 0))

    @pl.when(step == steps - 1)
    def _():
        logits[...] = acc[...].T


def spread_kernel(cols, weights, prior, halo, hslot, given, table, logits, prop, residue, errors, halo_tab, prop_all, onehot):
    step = pl.program_id(0)
    per = weights.shape[0]
    classes = prior.shape[1]

    @pl.when(step == 0)
    def _():
        slots = halo.shape[0]
        slot = lax.broadcasted_iota(jnp.int32, (slots, LANES), 0)
        for b in range(2):
            pick = (slot == hslot[b : b + 1, :]).astype(F32).astype(BF)
            halo_tab[b * LANES : (b + 1) * LANES, :] = dot(pick, halo[...], (0, 0)).astype(BF)

    for t in range(per):
        r = step * per + t
        acc = jnp.zeros((LANES, classes), F32)
        wide = jnp.zeros((LANES, LANES), F32)
        for m in range(4):
            pair = []
            for k in (2 * m, 2 * m + 1):
                wide = wide + weights[t, k].astype(F32)
                c = cols[r, k]
                if k < 6:
                    pair.append(prior[pl.ds(pl.multiple_of(c * LANES, LANES), LANES), :])
                else:
                    pair.append(halo_tab[pl.ds(pl.multiple_of((c - 16) * LANES, LANES), LANES), :])
            left = jnp.concatenate([weights[t, 2 * m], weights[t, 2 * m + 1]], axis=1)
            acc = acc + dot(left, jnp.concatenate(pair, axis=0), (1, 0))
        degree = jnp.sum(wide, axis=1, keepdims=True)
        mark = jnp.broadcast_to(given[pl.ds(r, 1), :], (LANES, LANES)).T
        lane = lax.broadcasted_iota(jnp.int32, (LANES, LANES), 1)
        seeds = jnp.concatenate([(mark == lane + g * LANES).astype(F32) for g in range(classes // LANES)], axis=1)
        mixed = (0.8 * (acc / degree) + 0.2 * seeds).astype(BF)
        prop[t * LANES : (t + 1) * LANES, :] = mixed
        prop_all[pl.ds(pl.multiple_of(r * LANES, LANES), LANES), :] = mixed

    @pl.when(step == pl.num_programs(0) - 1)
    def _():
        pick_rows(table, HALO_SLOTS, BATCH_SLOTS, prop_all.shape[0], onehot)
        lane = lax.broadcasted_iota(jnp.int32, (LANES, LANES), 1)
        out = jnp.zeros((LANES, LANES), F32)
        for s in range(BATCH_SLOTS):
            at = slice(s * LANES, (s + 1) * LANES)
            log_z = jnp.log(dot(onehot[at, :], prop_all[...], (1, 0)))
            target = log_z - jnp.mean(log_z, axis=1, keepdims=True)
            valid = table[:, HALO_SLOTS + s : HALO_SLOTS + s + 1] >= 0
            differ = jnp.where(valid, logits[at, :] - target, 0.0)
            out = jnp.where(lane == s, 0.5 * jnp.mean(differ * differ, axis=1, keepdims=True), out)
            residue[at, :] = (differ * (1.0 / 256.0)).astype(BF)
        errors[...] = out


def gradients(w_out, hidden, residue, x):
    h = hidden[...]
    wide = h.astype(F32)
    back = (dot(w_out[...], residue[...], (1, 1)) * (1.0 - wide * wide)).astype(BF)
    return dot(h, residue[...], (1, 0)), dot(back, x[...], (1, 0))


def peer_kernel(place, w_out, hidden, residue, x, grad):
    out, into = gradients(w_out, hidden, residue, x)
    grad[:, :512] = out.astype(BF)
    grad[:, 512:] = into.astype(BF)


def own_kernel(place, w_out, hidden, residue, x, arrived, errors, a, send_b, keep_b, send_c, keep_c, errors_to):
    out, into = gradients(w_out, hidden, residue, x)
    a[...] = (out + arrived[:, :512].astype(F32)).astype(BF)
    total = (into + arrived[:, 512:].astype(F32)).astype(BF)
    left = total[:, :512].reshape(2, 256, 512)
    right = total[:, 512:].reshape(4, 2, 64, 512)

    for half in range(2):

        @pl.when(place[1] == half)
        def _():
            keep_b[0] = left[half]
            send_b[0] = left[1 - half]

        @pl.when(place[2] == half)
        def _():
            keep_c[0] = right[:, half]
            send_c[0] = right[:, 1 - half]

    errors_to[...] = errors[...]


def pairing(level, dims):
    flip = 3 if level == 1 else 1
    pairs = []
    for source in range(128):
        core = source % 2
        spot = [source // 32, (source // 8) % 4, (source // 2) % 4]
        for d in dims:
            shifted = (spot[d] - (1 - core)) % 4
            spot[d] = ((shifted ^ flip) + (1 - core)) % 4
        pairs.append((source, ((spot[0] * 4 + spot[1]) * 4 + spot[2]) * 2 + core))
    return pairs


def exchange(x, level, dims):
    return lax.ppermute(x, DEV, pairing(level, dims))


def deal_kernel(bits, k0, r0, k1, r1, k2, r2, own, *sends):
    for m in range(8):
        a = bits[0] ^ (m >> 2)
        b = bits[1] ^ ((m >> 1) & 1)
        c = bits[2] ^ (m & 1)
        for j, (k, r) in enumerate(((k0, r0), (k1, r1), (k2, r2))):
            piece = k[a, b, c].astype(F32) + r[a, b, c].astype(F32)
            if m == 0:
                own[:, j * 512 : (j + 1) * 512] = piece
            else:
                sends[m - 1][:, j * 512 : (j + 1) * 512] = piece.astype(BF)


def summed_over_chips(first, second, halves, bits):
    shape_a, shape_b, shape_c = (2, 4, 4, UNITS, 512), (2, 2, 4, UNITS, 512), (2, 4, 2, UNITS, 512)
    send_a, send_b1, keep_b1, send_c1, keep_c1 = first
    keep_a, send_b2, keep_b2, send_c2, keep_c2 = second
    got_a = exchange(send_a, 1, (0,)).reshape(shape_a)
    got_b1, got_b2 = (exchange(v, 1, (1,)).reshape(shape_b) for v in (send_b1, send_b2))
    got_c1, got_c2 = (exchange(v, 1, (2,)).reshape(shape_c) for v in (send_c1, send_c2))
    keep_a = keep_a.reshape(shape_a)
    keep_b1, keep_b2 = keep_b1.reshape(shape_b), keep_b2.reshape(shape_b)
    keep_c1, keep_c2 = keep_c1.reshape(shape_c), keep_c2.reshape(shape_c)

    def added(kept, got, dim=None, half=None):
        if dim is not None:
            kept, got = (lax.dynamic_slice_in_dim(v, 2 * half, 2, dim) for v in (kept, got))
        return kept.astype(F32) + got.astype(F32)

    def sent(value, dim):
        return exchange(value.astype(BF), 1, (dim,))

    _, hb, hc = halves
    b_send = added(keep_b1, got_b1).astype(BF)
    b_got = sent(b_send, 0)
    a_got = sent(added(keep_a, got_a, 2, 1 - hc), 2)
    c_got = sent(jnp.stack([added(keep_c1, got_c1, 1, 1 - hb), added(keep_c2, got_c2, 1, 1 - hb)]), 1)
    b = added(keep_b2, got_b2).astype(BF)
    a = added(keep_a, got_a, 2, hc).astype(BF)
    c1 = added(keep_c1, got_c1, 1, hb).astype(BF)
    c2 = added(keep_c2, got_c2, 1, hb).astype(BF)
    b_last = sent(added(b, b_got, 2, 1 - hc), 2)
    a_last = sent(added(a, a_got, 1, 1 - hb), 1)
    c_last = sent(added(c1, c_got[0]), 0)
    b = added(b, b_got, 2, hc)
    a = added(a, a_got, 1, hb)
    c = added(c2, c_got[1])
    piece = jax.ShapeDtypeStruct((UNITS, 1536), BF)
    own, *pieces = pl.pallas_call(
        deal_kernel,
        in_specs=[pl.BlockSpec(memory_space=pltpu.SMEM)] + [pl.BlockSpec(memory_space=pltpu.VMEM)] * 6,
        out_shape=[jax.ShapeDtypeStruct((UNITS, 1536), F32)] + [piece] * 7,
        compiler_params=params(16),
        name="deal",
    )(bits, a, a_last, b, b_last, c, c_last)
    total = own
    for m in range(1, 8):
        dims = [d for d in range(3) if (m >> (2 - d)) & 1]
        total = total + exchange(pieces[m - 1], 2, dims).astype(F32)
    return total


def on_device(prior, label_class, labeled, features, tile_cols, tile_weights, halo_owner, halo_local, batch_owner, batch_local, w_in, w_out):
    nodes, classes = prior.shape
    feat = features.shape[1]
    hid = w_in.shape[0]
    halo_count = halo_local.shape[0]
    batch = batch_local.shape[0]
    rows = BATCH_SLOTS * LANES
    me = lax.axis_index(DEV)
    core = me % 2
    chip = (me // 32, (me // 8) % 4, (me // 2) % 4)
    spots = [(s + 3 + core) % 4 for s in chip]
    halves = [s // 2 for s in spots]
    peer_half = (chip[0] + 4 - core) % 4 // 2
    place = jnp.stack([*halves, core, peer_half]).astype(jnp.int32)
    bits = jnp.stack([s % 2 for s in spots]).astype(jnp.int32)
    vmem = pl.BlockSpec(memory_space=pltpu.VMEM)
    smem = pl.BlockSpec(memory_space=pltpu.SMEM)
    hbm = pl.BlockSpec(memory_space=pl.ANY)
    i32 = jnp.int32

    bo = batch_owner.reshape(batch // LANES, LANES)
    table, hslot, brank = pl.pallas_call(
        request_kernel,
        in_specs=[vmem] * 4,
        out_shape=[
            jax.ShapeDtypeStruct((LANES, LANES), i32),
            jax.ShapeDtypeStruct((halo_count // LANES, LANES), i32),
            jax.ShapeDtypeStruct((batch // LANES, LANES), i32),
        ],
        name="request",
    )(
        halo_owner.reshape(halo_count // LANES, LANES),
        halo_local.reshape(halo_count // LANES, LANES),
        bo,
        batch_local.reshape(batch // LANES, LANES),
    )
    asked = lax.all_to_all(table[:, : HALO_SLOTS + BATCH_SLOTS], DEV, 0, 0, tiled=True)

    served = prior[jnp.maximum(asked[:, :HALO_SLOTS], 0)]
    halo = lax.all_to_all(served, DEV, 0, 0, tiled=True).reshape(LANES * HALO_SLOTS, classes)

    def whole(shape):
        return pl.BlockSpec(shape, lambda i, *_: (0,) * len(shape))

    def once(shape):
        return pl.BlockSpec(shape, lambda i, *_: (0,) * len(shape), pipeline_mode=pl.Buffered(1))

    def rows_at(offset, width):
        return pl.BlockSpec((HBLK, width), lambda i, *_: (i + offset, 0))

    slots = HALO_SLOTS + BATCH_SLOTS
    chunks = HBLK // UNITS
    x, hidden, logits, w_out_o = pl.pallas_call(
        forward_kernel,
        grid=(hid // HBLK,),
        in_specs=[smem, once((LANES, slots)), once((nodes, feat)), hbm, hbm],
        out_specs=[whole((rows, feat)), rows_at(0, rows), whole((rows, classes)), rows_at(0, classes)],
        out_shape=[
            jax.ShapeDtypeStruct((rows, feat), BF),
            jax.ShapeDtypeStruct((hid, rows), BF),
            jax.ShapeDtypeStruct((rows, classes), F32),
            jax.ShapeDtypeStruct((hid, classes), BF),
        ],
        scratch_shapes=[
            pltpu.VMEM((rows, nodes), BF),
            pltpu.VMEM((classes, rows), F32),
            pltpu.VMEM((2, chunks, UNITS, feat), BF),
            pltpu.VMEM((2, chunks, UNITS, classes), BF),
            pltpu.SemaphoreType.DMA((2,)),
            pltpu.SemaphoreType.DMA((2,)),
        ],
        compiler_params=params(36),
        name="forward",
    )(place, asked, features, w_in.reshape(128, UNITS, feat), w_out.reshape(128, UNITS, classes))

    row_tiles = tile_weights.shape[0]
    per = 2
    given = jnp.where(labeled == 1, label_class, -1).reshape(row_tiles, LANES)
    prop, residue, errors = pl.pallas_call(
        spread_kernel,
        grid=(row_tiles // per,),
        in_specs=[
            smem,
            pl.BlockSpec((per, 8, LANES, LANES), lambda i: (i, 0, 0, 0)),
            once((nodes, classes)),
            once((LANES * HALO_SLOTS, classes)),
            once((halo_count // LANES, LANES)),
            once((row_tiles, LANES)),
            once((LANES, slots)),
            once((rows, classes)),
        ],
        out_specs=[
            pl.BlockSpec((per * LANES, classes), lambda i: (i, 0)),
            whole((rows, classes)),
            whole((LANES, LANES)),
        ],
        out_shape=[
            jax.ShapeDtypeStruct((nodes, classes), BF),
            jax.ShapeDtypeStruct((rows, classes), BF),
            jax.ShapeDtypeStruct((LANES, LANES), F32),
        ],
        scratch_shapes=[
            pltpu.VMEM((halo_count, classes), BF),
            pltpu.VMEM((nodes, classes), BF),
            pltpu.VMEM((rows, nodes), BF),
        ],
        compiler_params=params(24),
        name="spread",
    )(tile_cols, tile_weights, prior, halo, hslot, given, asked, logits)

    partner = [(d, d ^ 1) for d in range(128)]
    part_rows = 2 * HBLK

    def peer_part(part):
        def block(i, p):
            half = p[4] if part else 1 - p[4]
            return (2 * half + i, 0)

        grad = pl.pallas_call(
            peer_kernel,
            grid_spec=pltpu.PrefetchScalarGridSpec(
                num_scalar_prefetch=1,
                grid=(2,),
                in_specs=[
                    pl.BlockSpec((HBLK, classes), block),
                    pl.BlockSpec((HBLK, rows), block),
                    once((rows, classes)),
                    once((rows, feat)),
                ],
                out_specs=rows_at(0, classes + feat),
            ),
            out_shape=jax.ShapeDtypeStruct((part_rows, classes + feat), BF),
            compiler_params=params(24),
        )(place, w_out_o, hidden, residue, x)
        return lax.ppermute(grad, DEV, partner)

    b_spec = pl.BlockSpec((1, 256, 512), lambda i, p: (i, 0, 0))
    c_spec = pl.BlockSpec((1, 4, 64, 512), lambda i, p: (i, 0, 0, 0))
    b_shape = jax.ShapeDtypeStruct((2, 256, 512), BF)
    c_shape = jax.ShapeDtypeStruct((2, 4, 64, 512), BF)

    def own_part(part, arrived):
        def block(i, p):
            half = p[0] if part else 1 - p[0]
            return (4 + 2 * half + i, 0)

        return pl.pallas_call(
            own_kernel,
            grid_spec=pltpu.PrefetchScalarGridSpec(
                num_scalar_prefetch=1,
                grid=(2,),
                in_specs=[
                    pl.BlockSpec((HBLK, classes), block),
                    pl.BlockSpec((HBLK, rows), block),
                    once((rows, classes)),
                    once((rows, feat)),
                    rows_at(0, classes + feat),
                    once((LANES, LANES)),
                ],
                out_specs=[rows_at(0, classes), b_spec, b_spec, c_spec, c_spec, whole((LANES, LANES))],
            ),
            out_shape=[
                jax.ShapeDtypeStruct((part_rows, classes), BF),
                b_shape,
                b_shape,
                c_shape,
                c_shape,
                jax.ShapeDtypeStruct((LANES, LANES), F32),
            ],
            compiler_params=params(28),
        )(place, w_out_o, hidden, residue, x, arrived, errors)

    arrived = [peer_part(0), peer_part(1)]
    *first, _ = own_part(0, arrived[0])
    *second, errors_out = own_part(1, arrived[1])
    total = summed_over_chips(first, second, halves, bits)

    back_errors = lax.all_to_all(errors_out[:, :BATCH_SLOTS], DEV, 0, 0, tiled=True)
    row_error = pl.pallas_call(
        returned_kernel,
        in_specs=[vmem] * 3,
        out_shape=jax.ShapeDtypeStruct((batch // LANES, LANES), F32),
        name="returned",
    )(back_errors, bo, brank).reshape(batch)
    return prop, row_error, total[:, 512:], total[:, :512]


def solution(mesh):
    split = Mesh(mesh.devices.reshape(128), (DEV,))
    in_specs = (
        P(DEV, None),
        P(DEV),
        P(DEV),
        P(DEV, None),
        P(DEV, None),
        P(DEV, None, None, None),
        P(DEV, None),
        P(DEV),
        P(DEV, None),
        P(DEV),
        P(),
        P(),
    )
    out_specs = (P(DEV, None), P(DEV), P(DEV, None), P(DEV, None))
    return jax.shard_map(on_device, mesh=split, in_specs=in_specs, out_specs=out_specs, check_vma=False)
```

```python
import jax
import jax.numpy as jnp
from jax import lax
from jax.experimental import pallas as pl
from jax.experimental.pallas import tpu as pltpu
from jax.sharding import Mesh
from jax.sharding import PartitionSpec as P


DEV = "dev"
BF = jnp.bfloat16
F32 = jnp.float32
LANES = 128
HALO_SLOTS = 4
BATCH_SLOTS = 8
UNITS = 32
HBLK = 512


def params(mib=48, **more):
    return pltpu.CompilerParams(vmem_limit_bytes=mib * 2**20, **more)


def in_hbm(x):
    return pltpu.with_memory_space_constraint(x, pltpu.HBM)


def dot(left, right, dims):
    return lax.dot_general(left, right, ((dims[:1], dims[1:]), ((), ())), preferred_element_type=F32)


def ranks_of(owner_ref, blocks):
    below = lax.broadcasted_iota(jnp.int32, (LANES, LANES), 0)
    along = lax.broadcasted_iota(jnp.int32, (LANES, LANES), 1)
    rows = [owner_ref[b : b + 1, :] for b in range(blocks)]
    cols = [jnp.broadcast_to(row, (LANES, LANES)).T for row in rows]
    ranks = []
    for i in range(blocks):
        earlier = jnp.zeros((LANES, LANES), F32)
        for j in range(i + 1):
            same = cols[j] == rows[i]
            if j == i:
                same = same & (below < along)
            earlier = earlier + same.astype(F32)
        ranks.append(jnp.sum(earlier, axis=0, keepdims=True).astype(jnp.int32))
    return rows, ranks


def request_kernel(ho, hl, bo, bl, table, hslot, brank):
    device = lax.broadcasted_iota(jnp.int32, (LANES, LANES), 0)
    lane = lax.broadcasted_iota(jnp.int32, (LANES, LANES), 1)
    out = jnp.zeros((LANES, LANES), F32)
    at = 0
    for owner, local, count in ((ho, hl, HALO_SLOTS), (bo, bl, BATCH_SLOTS)):
        blocks = owner.shape[0]
        rows, ranks = ranks_of(owner, blocks)
        for s in range(count):
            total = jnp.zeros((LANES, LANES), F32)
            for i in range(blocks):
                hit = (device == rows[i]) & (ranks[i] == s)
                named = (local[i : i + 1, :] + 1).astype(F32)
                total = total + jnp.where(hit, jnp.broadcast_to(named, (LANES, LANES)), 0.0)
            out = jnp.where(lane == at, jnp.sum(total, axis=1, keepdims=True), out)
            at += 1
        for i in range(blocks):
            if owner is ho:
                hslot[i : i + 1, :] = rows[i] * HALO_SLOTS + ranks[i]
            else:
                brank[i : i + 1, :] = ranks[i]
    table[...] = out.astype(jnp.int32) - 1


def returned_kernel(errors, bo, brank, out):
    device = lax.broadcasted_iota(jnp.int32, (LANES, LANES), 0)
    for i in range(bo.shape[0]):
        total = jnp.zeros((LANES, LANES), F32)
        for s in range(BATCH_SLOTS):
            hit = (device == bo[i : i + 1, :]) & (brank[i : i + 1, :] == s)
            total = total + jnp.where(hit, errors[:, s : s + 1], 0.0)
        out[i : i + 1, :] = jnp.sum(total, axis=0, keepdims=True)


def pick_rows(table, first, count, nodes, onehot):
    node = lax.broadcasted_iota(jnp.int32, (LANES, nodes), 1)
    for s in range(count):
        wanted = table[:, first + s : first + s + 1]
        onehot[s * LANES : (s + 1) * LANES, :] = (node == wanted).astype(F32).astype(BF)


def forward_kernel(place, table, features, w_in, w_out, x, hidden, logits, w_out_to, onehot, acc, nodes_x, in_buf, out_buf, nodes_sem, in_sem, out_sem):
    step = pl.program_id(0)
    steps = pl.num_programs(0)
    chunks = HBLK // UNITS
    core = place[3]

    def fetch(block, slot):
        half = block // 4
        holder = jnp.where(half == 1, core, 1 - core)
        turn = 1 - holder
        a = (block % 4 + turn) % 4
        for n in range(chunks):
            b = (n // 4 + turn) % 4
            c = (n % 4 + turn) % 4
            source = ((a * 4 + b) * 4 + c) * 2 + holder
            pltpu.make_async_copy(w_in.at[source], in_buf.at[slot, n], in_sem.at[slot]).start()
            pltpu.make_async_copy(w_out.at[source], out_buf.at[slot, n], out_sem.at[slot]).start()

    @pl.when(step == 0)
    def _():
        whole = pltpu.make_async_copy(features, nodes_x, nodes_sem)
        whole.start()
        fetch(0, 0)
        pick_rows(table, HALO_SLOTS, BATCH_SLOTS, features.shape[0], onehot)
        whole.wait()
        x[...] = dot(onehot[...], nodes_x[...], (1, 0)).astype(BF)
        acc[...] = jnp.zeros(acc.shape, F32)

    slot = step % 2

    @pl.when(step + 1 < steps)
    def _():
        fetch(step + 1, 1 - slot)

    pltpu.make_async_copy(w_in.at[pl.ds(0, chunks)], in_buf.at[slot], in_sem.at[slot]).wait()
    pltpu.make_async_copy(w_out.at[pl.ds(0, chunks)], out_buf.at[slot], out_sem.at[slot]).wait()
    w_out_here = out_buf[slot].reshape(HBLK, out_buf.shape[3])
    w_out_to[...] = w_out_here
    h = jnp.tanh(dot(in_buf[slot].reshape(HBLK, in_buf.shape[3]), x[...], (1, 1))).astype(BF)
    hidden[...] = h
    acc[...] += dot(w_out_here, h, (0, 0))

    @pl.when(step == steps - 1)
    def _():
        logits[...] = acc[...].T


def spread_kernel(cols, weights, prior, halo, hslot, given, table, logits_far, prop, residue, errors, halo_tab, prop_all, onehot, logits, sem):
    step = pl.program_id(0)
    per = weights.shape[0]
    classes = prior.shape[1]

    fetch = pltpu.make_async_copy(logits_far, logits, sem)

    @pl.when(step == 0)
    def _():
        fetch.start()
        slots = halo.shape[0]
        slot = lax.broadcasted_iota(jnp.int32, (slots, LANES), 0)
        for b in range(2):
            pick = (slot == hslot[b : b + 1, :]).astype(F32).astype(BF)
            halo_tab[b * LANES : (b + 1) * LANES, :] = dot(pick, halo[...], (0, 0)).astype(BF)

    for t in range(per):
        r = step * per + t
        acc = jnp.zeros((LANES, classes), F32)
        wide = jnp.zeros((LANES, LANES), F32)
        for m in range(4):
            pair = []
            for k in (2 * m, 2 * m + 1):
                wide = wide + weights[t, k].astype(F32)
                c = cols[r, k]
                if k < 6:
                    pair.append(prior[pl.ds(pl.multiple_of(c * LANES, LANES), LANES), :])
                else:
                    pair.append(halo_tab[pl.ds(pl.multiple_of((c - 16) * LANES, LANES), LANES), :])
            left = jnp.concatenate([weights[t, 2 * m], weights[t, 2 * m + 1]], axis=1)
            acc = acc + dot(left, jnp.concatenate(pair, axis=0), (1, 0))
        degree = jnp.sum(wide, axis=1, keepdims=True)
        mark = jnp.broadcast_to(given[pl.ds(r, 1), :], (LANES, LANES)).T
        lane = lax.broadcasted_iota(jnp.int32, (LANES, LANES), 1)
        seeds = jnp.concatenate([(mark == lane + g * LANES).astype(F32) for g in range(classes // LANES)], axis=1)
        mixed = (0.8 * (acc / degree) + 0.2 * seeds).astype(BF)
        prop[t * LANES : (t + 1) * LANES, :] = mixed
        prop_all[pl.ds(pl.multiple_of(r * LANES, LANES), LANES), :] = mixed

    @pl.when(step == pl.num_programs(0) - 1)
    def _():
        pick_rows(table, HALO_SLOTS, BATCH_SLOTS, prop_all.shape[0], onehot)
        lane = lax.broadcasted_iota(jnp.int32, (LANES, LANES), 1)
        out = jnp.zeros((LANES, LANES), F32)
        fetch.wait()
        tall = 512
        for s in range(BATCH_SLOTS):
            at = slice(s * LANES, (s + 1) * LANES)
            if s % 4 == 0:
                picked = dot(onehot[s * LANES : s * LANES + tall, :], prop_all[...], (1, 0))
            log_z = jnp.log(picked[s % 4 * LANES : (s % 4 + 1) * LANES])
            target = log_z - jnp.mean(log_z, axis=1, keepdims=True)
            valid = table[:, HALO_SLOTS + s : HALO_SLOTS + s + 1] >= 0
            differ = jnp.where(valid, logits[at, :] - target, 0.0)
            out = jnp.where(lane == s, 0.5 * jnp.mean(differ * differ, axis=1, keepdims=True), out)
            residue[at, :] = (differ * (1.0 / 256.0)).astype(BF)
        errors[...] = out


def gradients(w_out, hidden, residue, x):
    h = hidden[...]
    wide = h.astype(F32)
    back = (dot(w_out[...], residue[...], (1, 1)) * (1.0 - wide * wide)).astype(BF)
    return dot(h, residue[...], (1, 0)), dot(back, x[...], (1, 0))


def peer_kernel(place, w_out, hidden, residue, x, grad):
    out, into = gradients(w_out, hidden, residue, x)
    grad[:, :512] = out.astype(BF)
    grad[:, 512:] = into.astype(BF)


def own_kernel(place, w_out, hidden, residue, x, arrived, errors, a, send_b, keep_b, send_c, keep_c, errors_to):
    out, into = gradients(w_out, hidden, residue, x)
    a[...] = (out + arrived[:, :512].astype(F32)).astype(BF)
    total = (into + arrived[:, 512:].astype(F32)).astype(BF)
    left = total[:, :512].reshape(2, 256, 512)
    right = total[:, 512:].reshape(4, 2, 64, 512)

    for half in range(2):

        @pl.when(place[1] == half)
        def _():
            keep_b[0] = left[half]
            send_b[0] = left[1 - half]

        @pl.when(place[2] == half)
        def _():
            keep_c[0] = right[:, half]
            send_c[0] = right[:, 1 - half]

    errors_to[...] = errors[...]


def pairing(level, dims):
    flip = 3 if level == 1 else 1
    pairs = []
    for source in range(128):
        core = source % 2
        spot = [source // 32, (source // 8) % 4, (source // 2) % 4]
        for d in dims:
            shifted = (spot[d] - (1 - core)) % 4
            spot[d] = ((shifted ^ flip) + (1 - core)) % 4
        pairs.append((source, ((spot[0] * 4 + spot[1]) * 4 + spot[2]) * 2 + core))
    return pairs


def exchange(x, level, dims):
    return lax.ppermute(x, DEV, pairing(level, dims))


def corners():
    groups = []
    for core in range(2):
        for high in range(8):
            group = []
            for low in range(8):
                shifted = [2 * ((high >> (2 - d)) & 1) + ((low >> (2 - d)) & 1) for d in range(3)]
                a, b, c = ((v + 1 - core) % 4 for v in shifted)
                group.append(((a * 4 + b) * 4 + c) * 2 + core)
            groups.append(group)
    return groups


def deal_kernel(k0, r0, k1, r1, k2, r2, pieces):
    for m in range(8):
        at = (m >> 2, (m >> 1) & 1, m & 1)
        for j, (k, r) in enumerate(((k0, r0), (k1, r1), (k2, r2))):
            piece = k[at].astype(F32) + r[at].astype(F32)
            pieces[m, :, j * 512 : (j + 1) * 512] = piece.astype(BF)


def summed_over_chips(first, second, halves):
    shape_a, shape_b, shape_c = (2, 4, 4, UNITS, 512), (2, 2, 4, UNITS, 512), (2, 4, 2, UNITS, 512)
    send_a, send_b1, keep_b1, send_c1, keep_c1 = first
    keep_a, send_b2, keep_b2, send_c2, keep_c2 = second
    got_c1 = exchange(send_c1, 1, (2,)).reshape(shape_c)
    got_b1 = exchange(send_b1, 1, (1,)).reshape(shape_b)
    got_a = exchange(send_a, 1, (0,)).reshape(shape_a)
    got_c2 = exchange(send_c2, 1, (2,)).reshape(shape_c)
    got_b2 = exchange(send_b2, 1, (1,)).reshape(shape_b)
    keep_a = keep_a.reshape(shape_a)
    keep_b1, keep_b2 = keep_b1.reshape(shape_b), keep_b2.reshape(shape_b)
    keep_c1, keep_c2 = keep_c1.reshape(shape_c), keep_c2.reshape(shape_c)

    def added(kept, got, dim=None, half=None):
        if dim is not None:
            kept, got = (lax.dynamic_slice_in_dim(v, 2 * half, 2, dim) for v in (kept, got))
        return kept.astype(F32) + got.astype(F32)

    def sent(value, dim):
        return exchange(value.astype(BF), 1, (dim,))

    _, hb, hc = halves
    b_send = added(keep_b1, got_b1).astype(BF)
    b_got = sent(b_send, 0)
    a_got = sent(added(keep_a, got_a, 2, 1 - hc), 2)
    c_got = sent(jnp.stack([added(keep_c1, got_c1, 1, 1 - hb), added(keep_c2, got_c2, 1, 1 - hb)]), 1)
    b = added(keep_b2, got_b2).astype(BF)
    a = added(keep_a, got_a, 2, hc).astype(BF)
    c1 = added(keep_c1, got_c1, 1, hb).astype(BF)
    c2 = added(keep_c2, got_c2, 1, hb).astype(BF)
    b_last = sent(added(b, b_got, 2, 1 - hc), 2)
    a_last = sent(added(a, a_got, 1, 1 - hb), 1)
    c_last = sent(added(c1, c_got[0]), 0)
    b = added(b, b_got, 2, hc)
    a = added(a, a_got, 1, hb)
    c = added(c2, c_got[1])
    pieces = pl.pallas_call(
        deal_kernel,
        in_specs=[pl.BlockSpec(memory_space=pltpu.VMEM)] * 6,
        out_specs=pl.BlockSpec(memory_space=pltpu.VMEM),
        out_shape=jax.ShapeDtypeStruct((8, UNITS, 1536), BF),
        compiler_params=params(16),
        name="deal",
    )(a, a_last, b, b_last, c, c_last)
    dealt = lax.all_to_all(pieces, DEV, 0, 0, axis_index_groups=corners(), tiled=True)
    return jnp.sum(dealt.astype(F32), axis=0)


def on_device(prior, label_class, labeled, features, tile_cols, tile_weights, halo_owner, halo_local, batch_owner, batch_local, w_in, w_out):
    nodes, classes = prior.shape
    feat = features.shape[1]
    hid = w_in.shape[0]
    halo_count = halo_local.shape[0]
    batch = batch_local.shape[0]
    rows = BATCH_SLOTS * LANES
    me = lax.axis_index(DEV)
    core = me % 2
    chip = (me // 32, (me // 8) % 4, (me // 2) % 4)
    spots = [(s + 3 + core) % 4 for s in chip]
    halves = [s // 2 for s in spots]
    peer_half = (chip[0] + 4 - core) % 4 // 2
    place = jnp.stack([*halves, core, peer_half]).astype(jnp.int32)
    vmem = pl.BlockSpec(memory_space=pltpu.VMEM)
    smem = pl.BlockSpec(memory_space=pltpu.SMEM)
    hbm = pl.BlockSpec(memory_space=pl.ANY)
    i32 = jnp.int32

    bo = batch_owner.reshape(batch // LANES, LANES)
    table, hslot, brank = pl.pallas_call(
        request_kernel,
        in_specs=[vmem] * 4,
        out_shape=[
            jax.ShapeDtypeStruct((LANES, LANES), i32),
            jax.ShapeDtypeStruct((halo_count // LANES, LANES), i32),
            jax.ShapeDtypeStruct((batch // LANES, LANES), i32),
        ],
        name="request",
    )(
        halo_owner.reshape(halo_count // LANES, LANES),
        halo_local.reshape(halo_count // LANES, LANES),
        bo,
        batch_local.reshape(batch // LANES, LANES),
    )
    asked = lax.all_to_all(table[:, : HALO_SLOTS + BATCH_SLOTS], DEV, 0, 0, tiled=True)

    served = prior[jnp.maximum(asked[:, :HALO_SLOTS], 0)]
    halo = lax.all_to_all(served, DEV, 0, 0, tiled=True).reshape(LANES * HALO_SLOTS, classes)

    def whole(shape):
        return pl.BlockSpec(shape, lambda i, *_: (0,) * len(shape))

    def once(shape):
        return pl.BlockSpec(shape, lambda i, *_: (0,) * len(shape), pipeline_mode=pl.Buffered(1))

    def rows_at(offset, width):
        return pl.BlockSpec((HBLK, width), lambda i, *_: (i + offset, 0))

    slots = HALO_SLOTS + BATCH_SLOTS
    chunks = HBLK // UNITS
    x, hidden, logits, w_out_o = pl.pallas_call(
        forward_kernel,
        grid=(hid // HBLK,),
        in_specs=[smem, once((LANES, slots)), hbm, hbm, hbm],
        out_specs=[whole((rows, feat)), rows_at(0, rows), whole((rows, classes)), rows_at(0, classes)],
        out_shape=[
            jax.ShapeDtypeStruct((rows, feat), BF),
            pltpu.HBM((hid, rows), BF),
            pltpu.HBM((rows, classes), F32),
            pltpu.HBM((hid, classes), BF),
        ],
        scratch_shapes=[
            pltpu.VMEM((rows, nodes), BF),
            pltpu.VMEM((classes, rows), F32),
            pltpu.VMEM((nodes, feat), BF),
            pltpu.VMEM((2, chunks, UNITS, feat), BF),
            pltpu.VMEM((2, chunks, UNITS, classes), BF),
            pltpu.SemaphoreType.DMA,
            pltpu.SemaphoreType.DMA((2,)),
            pltpu.SemaphoreType.DMA((2,)),
        ],
        compiler_params=params(36),
        name="forward",
    )(
        place,
        asked,
        in_hbm(features),
        in_hbm(w_in.reshape(128, UNITS, feat)),
        in_hbm(w_out.reshape(128, UNITS, classes)),
    )

    row_tiles = tile_weights.shape[0]
    per = 2
    given = jnp.where(labeled == 1, label_class, -1).reshape(row_tiles, LANES)
    prop, residue, errors = pl.pallas_call(
        spread_kernel,
        grid=(row_tiles // per,),
        in_specs=[
            smem,
            pl.BlockSpec((per, 8, LANES, LANES), lambda i: (i, 0, 0, 0)),
            once((nodes, classes)),
            once((LANES * HALO_SLOTS, classes)),
            once((halo_count // LANES, LANES)),
            once((row_tiles, LANES)),
            once((LANES, slots)),
            hbm,
        ],
        out_specs=[
            pl.BlockSpec((per * LANES, classes), lambda i: (i, 0)),
            whole((rows, classes)),
            whole((LANES, LANES)),
        ],
        out_shape=[
            jax.ShapeDtypeStruct((nodes, classes), BF),
            jax.ShapeDtypeStruct((rows, classes), BF),
            jax.ShapeDtypeStruct((LANES, LANES), F32),
        ],
        scratch_shapes=[
            pltpu.VMEM((halo_count, classes), BF),
            pltpu.VMEM((nodes, classes), BF),
            pltpu.VMEM((rows, nodes), BF),
            pltpu.VMEM((rows, classes), F32),
            pltpu.SemaphoreType.DMA,
        ],
        compiler_params=params(24),
        name="spread",
    )(tile_cols, in_hbm(tile_weights), in_hbm(prior), halo, hslot, given, asked, in_hbm(logits))

    partner = [(d, d ^ 1) for d in range(128)]
    part_rows = 2 * HBLK

    def peer_part(part):
        def block(i, p):
            half = p[4] if part else 1 - p[4]
            return (2 * half + i, 0)

        grad = pl.pallas_call(
            peer_kernel,
            grid_spec=pltpu.PrefetchScalarGridSpec(
                num_scalar_prefetch=1,
                grid=(2,),
                in_specs=[
                    pl.BlockSpec((HBLK, classes), block),
                    pl.BlockSpec((HBLK, rows), block),
                    once((rows, classes)),
                    once((rows, feat)),
                ],
                out_specs=rows_at(0, classes + feat),
            ),
            out_shape=jax.ShapeDtypeStruct((part_rows, classes + feat), BF),
            compiler_params=params(24),
        )(place, in_hbm(w_out_o), in_hbm(hidden), residue, x)
        return lax.ppermute(grad, DEV, partner)

    b_spec = pl.BlockSpec((1, 256, 512), lambda i, p: (i, 0, 0))
    c_spec = pl.BlockSpec((1, 4, 64, 512), lambda i, p: (i, 0, 0, 0))
    b_shape = pltpu.HBM((2, 256, 512), BF)
    c_shape = pltpu.HBM((2, 4, 64, 512), BF)

    def own_part(part, arrived):
        def block(i, p):
            half = p[0] if part else 1 - p[0]
            return (4 + 2 * half + i, 0)

        return pl.pallas_call(
            own_kernel,
            grid_spec=pltpu.PrefetchScalarGridSpec(
                num_scalar_prefetch=1,
                grid=(2,),
                in_specs=[
                    pl.BlockSpec((HBLK, classes), block),
                    pl.BlockSpec((HBLK, rows), block),
                    once((rows, classes)),
                    once((rows, feat)),
                    rows_at(0, classes + feat),
                    once((LANES, LANES)),
                ],
                out_specs=[rows_at(0, classes), b_spec, b_spec, c_spec, c_spec, whole((LANES, LANES))],
            ),
            out_shape=[
                pltpu.HBM((part_rows, classes), BF),
                b_shape,
                b_shape,
                c_shape,
                c_shape,
                jax.ShapeDtypeStruct((LANES, LANES), F32),
            ],
            compiler_params=params(28),
        )(place, in_hbm(w_out_o), in_hbm(hidden), residue, x, arrived, errors)

    arrived = [peer_part(0), peer_part(1)]
    *first, _ = own_part(0, arrived[0])
    *second, errors_out = own_part(1, arrived[1])
    total = summed_over_chips(first, second, halves)

    back_errors = lax.all_to_all(errors_out[:, :BATCH_SLOTS], DEV, 0, 0, tiled=True)
    row_error = pl.pallas_call(
        returned_kernel,
        in_specs=[vmem] * 3,
        out_shape=jax.ShapeDtypeStruct((batch // LANES, LANES), F32),
        name="returned",
    )(back_errors, bo, brank).reshape(batch)
    return prop, row_error, total[:, 512:], total[:, :512]


def solution(mesh):
    split = Mesh(mesh.devices.reshape(128), (DEV,))
    in_specs = (
        P(DEV, None),
        P(DEV),
        P(DEV),
        P(DEV, None),
        P(DEV, None),
        P(DEV, None, None, None),
        P(DEV, None),
        P(DEV),
        P(DEV, None),
        P(DEV),
        P(),
        P(),
    )
    out_specs = (P(DEV, None), P(DEV), P(DEV, None), P(DEV, None))
    return jax.shard_map(on_device, mesh=split, in_specs=in_specs, out_specs=out_specs, check_vma=False)
```

```python
from functools import partial

import jax
import jax.numpy as jnp
from jax import lax
from jax.experimental import pallas as pl
from jax.experimental.pallas import tpu as pltpu
from jax.sharding import Mesh
from jax.sharding import PartitionSpec as P


DEV = "dev"
BF = jnp.bfloat16
F32 = jnp.float32
LANES = 128
HALO_SLOTS = 4
BATCH_SLOTS = 8
UNITS = 32
HBLK = 512


def params(mib=48, **more):
    return pltpu.CompilerParams(vmem_limit_bytes=mib * 2**20, **more)


def cost(gigaflops, mib, gigaexp=0.0):
    return pl.CostEstimate(flops=int(gigaflops * 1e9), bytes_accessed=int(mib * 2**20), transcendentals=int(gigaexp * 1e9))


def in_hbm(x):
    return pltpu.with_memory_space_constraint(x, pltpu.HBM)


def dot(left, right, dims):
    return lax.dot_general(left, right, ((dims[:1], dims[1:]), ((), ())), preferred_element_type=F32)


def ranks_of(owner_ref, blocks):
    below = lax.broadcasted_iota(jnp.int32, (LANES, LANES), 0)
    along = lax.broadcasted_iota(jnp.int32, (LANES, LANES), 1)
    rows = [owner_ref[b : b + 1, :] for b in range(blocks)]
    cols = [jnp.broadcast_to(row, (LANES, LANES)).T for row in rows]
    ranks = []
    for i in range(blocks):
        earlier = jnp.zeros((LANES, LANES), F32)
        for j in range(i + 1):
            same = cols[j] == rows[i]
            if j == i:
                same = same & (below < along)
            earlier = earlier + same.astype(F32)
        ranks.append(jnp.sum(earlier, axis=0, keepdims=True).astype(jnp.int32))
    return rows, ranks


def request_kernel(ho, hl, bo, bl, table, hslot, brank):
    device = lax.broadcasted_iota(jnp.int32, (LANES, LANES), 0)
    lane = lax.broadcasted_iota(jnp.int32, (LANES, LANES), 1)
    out = jnp.zeros((LANES, LANES), F32)
    at = 0
    for owner, local, count in ((ho, hl, HALO_SLOTS), (bo, bl, BATCH_SLOTS)):
        blocks = owner.shape[0]
        rows, ranks = ranks_of(owner, blocks)
        for s in range(count):
            total = jnp.zeros((LANES, LANES), F32)
            for i in range(blocks):
                hit = (device == rows[i]) & (ranks[i] == s)
                named = (local[i : i + 1, :] + 1).astype(F32)
                total = total + jnp.where(hit, jnp.broadcast_to(named, (LANES, LANES)), 0.0)
            out = jnp.where(lane == at, jnp.sum(total, axis=1, keepdims=True), out)
            at += 1
        for i in range(blocks):
            if owner is ho:
                hslot[i : i + 1, :] = rows[i] * HALO_SLOTS + ranks[i]
            else:
                brank[i : i + 1, :] = ranks[i]
    table[...] = out.astype(jnp.int32) - 1


def returned_kernel(errors, bo, brank, out):
    device = lax.broadcasted_iota(jnp.int32, (LANES, LANES), 0)
    for i in range(bo.shape[0]):
        total = jnp.zeros((LANES, LANES), F32)
        for s in range(BATCH_SLOTS):
            hit = (device == bo[i : i + 1, :]) & (brank[i : i + 1, :] == s)
            total = total + jnp.where(hit, errors[:, s : s + 1], 0.0)
        out[i : i + 1, :] = jnp.sum(total, axis=0, keepdims=True)


def pick_rows(table, first, count, nodes, onehot):
    node = lax.broadcasted_iota(jnp.int32, (LANES, nodes), 1)
    for s in range(count):
        wanted = table[:, first + s : first + s + 1]
        onehot[s * LANES : (s + 1) * LANES, :] = (node == wanted).astype(F32).astype(BF)


def forward_kernel(place, table, features, w_in, w_out, x, hidden, logits, w_out_to, onehot, acc, nodes_x, in_buf, out_buf, nodes_sem, in_sem, out_sem):
    step = pl.program_id(0)
    steps = pl.num_programs(0)
    chunks = HBLK // UNITS
    core = place[3]

    def fetch(block, slot):
        half = block // 4
        holder = jnp.where(half == 1, core, 1 - core)
        turn = 1 - holder
        a = (block % 4 + turn) % 4
        for n in range(chunks):
            b = (n // 4 + turn) % 4
            c = (n % 4 + turn) % 4
            source = ((a * 4 + b) * 4 + c) * 2 + holder
            pltpu.make_async_copy(w_in.at[source], in_buf.at[slot, n], in_sem.at[slot]).start()
            pltpu.make_async_copy(w_out.at[source], out_buf.at[slot, n], out_sem.at[slot]).start()

    @pl.when(step == 0)
    def _():
        whole = pltpu.make_async_copy(features, nodes_x, nodes_sem)
        whole.start()
        fetch(0, 0)
        pick_rows(table, HALO_SLOTS, BATCH_SLOTS, features.shape[0], onehot)
        whole.wait()
        x[...] = dot(onehot[...], nodes_x[...], (1, 0)).astype(BF)
        acc[...] = jnp.zeros(acc.shape, F32)

    slot = step % 2

    @pl.when(step + 1 < steps)
    def _():
        fetch(step + 1, 1 - slot)

    pltpu.make_async_copy(w_in.at[pl.ds(0, chunks)], in_buf.at[slot], in_sem.at[slot]).wait()
    pltpu.make_async_copy(w_out.at[pl.ds(0, chunks)], out_buf.at[slot], out_sem.at[slot]).wait()
    w_out_here = out_buf[slot].reshape(HBLK, out_buf.shape[3])
    w_out_to[...] = w_out_here
    h = jnp.tanh(dot(in_buf[slot].reshape(HBLK, in_buf.shape[3]), x[...], (1, 1))).astype(BF)
    hidden[...] = h
    acc[...] += dot(w_out_here, h, (0, 0))

    @pl.when(step == steps - 1)
    def _():
        logits[...] = acc[...].T


def spread_kernel(
    cols, weights, prior_far, halo, hslot, given, table, logits_far, hidden_far, w_out_far,
    prop, residue, errors, hidden, w_out,
    halo_tab, prop_all, onehot, prior, logits, sems,
):
    step = pl.program_id(0)
    per = weights.shape[0]
    classes = prior.shape[1]
    pairs = ((prior_far, prior), (logits_far, logits), (w_out_far, w_out), (hidden_far, hidden))
    copies = [pltpu.make_async_copy(far, near, sems.at[n]) for n, (far, near) in enumerate(pairs)]

    @pl.when(step == 0)
    def _():
        for copy in copies:
            copy.start()
        owner = lax.broadcasted_iota(jnp.int32, (LANES, LANES), 0) * HALO_SLOTS
        for b in range(2):
            near = jnp.zeros((LANES, classes), F32)
            for k in range(HALO_SLOTS):
                pick = (owner + k == hslot[b : b + 1, :]).astype(F32).astype(BF)
                near = near + dot(pick, halo[:, k, :], (0, 0))
            halo_tab[b * LANES : (b + 1) * LANES, :] = near.astype(BF)
        copies[0].wait()

    for t in range(per):
        r = step * per + t
        acc = jnp.zeros((LANES, classes), F32)
        wide = jnp.zeros((LANES, LANES), F32)
        for m in range(4):
            pair = []
            for k in (2 * m, 2 * m + 1):
                wide = wide + weights[t, k].astype(F32)
                c = cols[r, k]
                if k < 6:
                    pair.append(prior[pl.ds(pl.multiple_of(c * LANES, LANES), LANES), :])
                else:
                    pair.append(halo_tab[pl.ds(pl.multiple_of((c - 16) * LANES, LANES), LANES), :])
            left = jnp.concatenate([weights[t, 2 * m], weights[t, 2 * m + 1]], axis=1)
            acc = acc + dot(left, jnp.concatenate(pair, axis=0), (1, 0))
        degree = jnp.sum(wide, axis=1, keepdims=True)
        mark = jnp.broadcast_to(given[pl.ds(r, 1), :], (LANES, LANES)).T
        lane = lax.broadcasted_iota(jnp.int32, (LANES, LANES), 1)
        seeds = jnp.concatenate([(mark == lane + g * LANES).astype(F32) for g in range(classes // LANES)], axis=1)
        mixed = (0.8 * (acc / degree) + 0.2 * seeds).astype(BF)
        prop[t * LANES : (t + 1) * LANES, :] = mixed
        prop_all[pl.ds(pl.multiple_of(r * LANES, LANES), LANES), :] = mixed

    @pl.when(step == pl.num_programs(0) - 1)
    def _():
        pick_rows(table, HALO_SLOTS, BATCH_SLOTS, prop_all.shape[0], onehot)
        lane = lax.broadcasted_iota(jnp.int32, (LANES, LANES), 1)
        out = jnp.zeros((LANES, LANES), F32)
        copies[1].wait()
        tall = 512
        for s in range(BATCH_SLOTS):
            at = slice(s * LANES, (s + 1) * LANES)
            if s % 4 == 0:
                picked = dot(onehot[s * LANES : s * LANES + tall, :], prop_all[...], (1, 0))
            log_z = jnp.log(picked[s % 4 * LANES : (s % 4 + 1) * LANES])
            target = log_z - jnp.mean(log_z, axis=1, keepdims=True)
            valid = table[:, HALO_SLOTS + s : HALO_SLOTS + s + 1] >= 0
            differ = jnp.where(valid, logits[at, :] - target, 0.0)
            out = jnp.where(lane == s, 0.5 * jnp.mean(differ * differ, axis=1, keepdims=True), out)
            residue[at, :] = (differ * (1.0 / 256.0)).astype(BF)
        errors[...] = out
        copies[2].wait()
        copies[3].wait()


def gradients(block, w_out, hidden, residue, x):
    at = pl.ds(pl.multiple_of(block * HBLK, HBLK), HBLK)
    h = hidden[at, :]
    wide = h.astype(F32)
    back = (dot(w_out[at, :], residue[...], (1, 1)) * (1.0 - wide * wide)).astype(BF)
    return dot(h, residue[...], (1, 0)), dot(back, x[...], (1, 0))


def peer_kernel(part, place, w_out, hidden, residue, x, grad):
    half = place[4] if part else 1 - place[4]
    out, into = gradients(2 * half + pl.program_id(0), w_out, hidden, residue, x)
    grad[:, :512] = out.astype(BF)
    grad[:, 512:] = into.astype(BF)


def own_kernel(part, place, w_out, hidden, residue, x, arrived, errors, a, send_b, keep_b, send_c, keep_c, errors_to):
    half = place[0] if part else 1 - place[0]
    out, into = gradients(4 + 2 * half + pl.program_id(0), w_out, hidden, residue, x)
    a[...] = (out + arrived[:, :512].astype(F32)).astype(BF)
    total = (into + arrived[:, 512:].astype(F32)).astype(BF)
    left = total[:, :512].reshape(2, 256, 512)
    right = total[:, 512:].reshape(4, 2, 64, 512)

    for half in range(2):

        @pl.when(place[1] == half)
        def _():
            keep_b[0] = left[half]
            send_b[0] = left[1 - half]

        @pl.when(place[2] == half)
        def _():
            keep_c[0] = right[:, half]
            send_c[0] = right[:, 1 - half]

    errors_to[...] = errors[...]


def pairing(level, dims):
    flip = 3 if level == 1 else 1
    pairs = []
    for source in range(128):
        core = source % 2
        spot = [source // 32, (source // 8) % 4, (source // 2) % 4]
        for d in dims:
            shifted = (spot[d] - (1 - core)) % 4
            spot[d] = ((shifted ^ flip) + (1 - core)) % 4
        pairs.append((source, ((spot[0] * 4 + spot[1]) * 4 + spot[2]) * 2 + core))
    return pairs


def exchange(x, level, dims):
    return lax.ppermute(x, DEV, pairing(level, dims))


def corners():
    groups = []
    for core in range(2):
        for high in range(8):
            group = []
            for low in range(8):
                shifted = [2 * ((high >> (2 - d)) & 1) + ((low >> (2 - d)) & 1) for d in range(3)]
                a, b, c = ((v + 1 - core) % 4 for v in shifted)
                group.append(((a * 4 + b) * 4 + c) * 2 + core)
            groups.append(group)
    return groups


def deal_kernel(k0, r0, k1, r1, k2, r2, pieces):
    for m in range(8):
        at = (m >> 2, (m >> 1) & 1, m & 1)
        for j, (k, r) in enumerate(((k0, r0), (k1, r1), (k2, r2))):
            piece = k[at].astype(F32) + r[at].astype(F32)
            pieces[m, :, j * 512 : (j + 1) * 512] = piece.astype(BF)


def summed_over_chips(first, second, halves):
    shape_a, shape_b, shape_c = (2, 4, 4, UNITS, 512), (2, 2, 4, UNITS, 512), (2, 4, 2, UNITS, 512)
    send_a, send_b1, keep_b1, send_c1, keep_c1 = first
    keep_a, send_b2, keep_b2, send_c2, keep_c2 = second
    got_c1 = exchange(send_c1, 1, (2,)).reshape(shape_c)
    got_b1 = exchange(send_b1, 1, (1,)).reshape(shape_b)
    got_a = exchange(send_a, 1, (0,)).reshape(shape_a)
    got_c2 = exchange(send_c2, 1, (2,)).reshape(shape_c)
    got_b2 = exchange(send_b2, 1, (1,)).reshape(shape_b)
    keep_a = keep_a.reshape(shape_a)
    keep_b1, keep_b2 = keep_b1.reshape(shape_b), keep_b2.reshape(shape_b)
    keep_c1, keep_c2 = keep_c1.reshape(shape_c), keep_c2.reshape(shape_c)

    def added(kept, got, dim=None, half=None):
        if dim is not None:
            kept, got = (lax.dynamic_slice_in_dim(v, 2 * half, 2, dim) for v in (kept, got))
        return kept.astype(F32) + got.astype(F32)

    def sent(value, dim):
        return exchange(value.astype(BF), 1, (dim,))

    _, hb, hc = halves
    b_send = added(keep_b1, got_b1).astype(BF)
    b_got = sent(b_send, 0)
    a_got = sent(added(keep_a, got_a, 2, 1 - hc), 2)
    c_got = sent(jnp.stack([added(keep_c1, got_c1, 1, 1 - hb), added(keep_c2, got_c2, 1, 1 - hb)]), 1)
    b = added(keep_b2, got_b2).astype(BF)
    a = added(keep_a, got_a, 2, hc).astype(BF)
    c1 = added(keep_c1, got_c1, 1, hb).astype(BF)
    c2 = added(keep_c2, got_c2, 1, hb).astype(BF)
    b_last = sent(added(b, b_got, 2, 1 - hc), 2)
    a_last = sent(added(a, a_got, 1, 1 - hb), 1)
    c_last = sent(added(c1, c_got[0]), 0)
    b = added(b, b_got, 2, hc)
    a = added(a, a_got, 1, hb)
    c = added(c2, c_got[1])
    pieces = pl.pallas_call(
        deal_kernel,
        in_specs=[pl.BlockSpec(memory_space=pltpu.VMEM)] * 6,
        out_specs=pl.BlockSpec(memory_space=pltpu.VMEM),
        out_shape=jax.ShapeDtypeStruct((8, UNITS, 1536), BF),
        compiler_params=params(16),
        name="deal",
    )(a, a_last, b, b_last, c, c_last)
    dealt = lax.all_to_all(pieces, DEV, 0, 0, axis_index_groups=corners(), tiled=True)
    return jnp.sum(dealt.astype(F32), axis=0)


def on_device(prior, label_class, labeled, features, tile_cols, tile_weights, halo_owner, halo_local, batch_owner, batch_local, w_in, w_out):
    nodes, classes = prior.shape
    feat = features.shape[1]
    hid = w_in.shape[0]
    halo_count = halo_local.shape[0]
    batch = batch_local.shape[0]
    rows = BATCH_SLOTS * LANES
    me = lax.axis_index(DEV)
    core = me % 2
    chip = (me // 32, (me // 8) % 4, (me // 2) % 4)
    spots = [(s + 3 + core) % 4 for s in chip]
    halves = [s // 2 for s in spots]
    peer_half = (chip[0] + 4 - core) % 4 // 2
    place = jnp.stack([*halves, core, peer_half]).astype(jnp.int32)
    vmem = pl.BlockSpec(memory_space=pltpu.VMEM)
    smem = pl.BlockSpec(memory_space=pltpu.SMEM)
    hbm = pl.BlockSpec(memory_space=pl.ANY)
    i32 = jnp.int32

    bo = batch_owner.reshape(batch // LANES, LANES)
    table, hslot, brank = pl.pallas_call(
        request_kernel,
        in_specs=[vmem] * 4,
        out_shape=[
            jax.ShapeDtypeStruct((LANES, LANES), i32),
            jax.ShapeDtypeStruct((halo_count // LANES, LANES), i32),
            jax.ShapeDtypeStruct((batch // LANES, LANES), i32),
        ],
        name="request",
    )(
        halo_owner.reshape(halo_count // LANES, LANES),
        halo_local.reshape(halo_count // LANES, LANES),
        bo,
        batch_local.reshape(batch // LANES, LANES),
    )
    asked = lax.all_to_all(table[:, : HALO_SLOTS + BATCH_SLOTS], DEV, 0, 0, tiled=True)

    served = prior[jnp.maximum(asked[:, :HALO_SLOTS], 0)]
    halo = lax.all_to_all(served, DEV, 0, 0, tiled=True)

    def whole(shape):
        return pl.BlockSpec(shape, lambda i, *_: (0,) * len(shape))

    def once(shape):
        return pl.BlockSpec(shape, lambda i, *_: (0,) * len(shape), pipeline_mode=pl.Buffered(1))

    def rows_at(offset, width):
        return pl.BlockSpec((HBLK, width), lambda i, *_: (i + offset, 0))

    slots = HALO_SLOTS + BATCH_SLOTS
    chunks = HBLK // UNITS
    x, hidden, logits, w_out_o = pl.pallas_call(
        forward_kernel,
        grid=(hid // HBLK,),
        in_specs=[smem, once((LANES, slots)), hbm, hbm, hbm],
        out_specs=[vmem, rows_at(0, rows), whole((rows, classes)), rows_at(0, classes)],
        out_shape=[
            pltpu.VMEM((rows, feat), BF),
            pltpu.HBM((hid, rows), BF),
            pltpu.HBM((rows, classes), F32),
            pltpu.HBM((hid, classes), BF),
        ],
        scratch_shapes=[
            pltpu.VMEM((rows, nodes), BF),
            pltpu.VMEM((classes, rows), F32),
            pltpu.VMEM((nodes, feat), BF),
            pltpu.VMEM((2, chunks, UNITS, feat), BF),
            pltpu.VMEM((2, chunks, UNITS, classes), BF),
            pltpu.SemaphoreType.DMA,
            pltpu.SemaphoreType.DMA((2,)),
            pltpu.SemaphoreType.DMA((2,)),
        ],
        compiler_params=params(32),
        cost_estimate=cost(17.2, 30, 0.0042),
        name="forward",
    )(
        place,
        asked,
        in_hbm(features),
        in_hbm(w_in.reshape(128, UNITS, feat)),
        in_hbm(w_out.reshape(128, UNITS, classes)),
    )

    row_tiles = tile_weights.shape[0]
    per = 2
    given = jnp.where(labeled == 1, label_class, -1).reshape(row_tiles, LANES)
    prop, residue, errors, hidden, w_out_o = pl.pallas_call(
        spread_kernel,
        grid=(row_tiles // per,),
        in_specs=[
            smem,
            pl.BlockSpec((per, 8, LANES, LANES), lambda i: (i, 0, 0, 0)),
            hbm,
            once((LANES, HALO_SLOTS, classes)),
            once((halo_count // LANES, LANES)),
            once((row_tiles, LANES)),
            once((LANES, slots)),
            hbm,
            hbm,
            hbm,
        ],
        out_specs=[
            pl.BlockSpec((per * LANES, classes), lambda i: (i, 0)),
            vmem,
            whole((LANES, LANES)),
            vmem,
            vmem,
        ],
        out_shape=[
            jax.ShapeDtypeStruct((nodes, classes), BF),
            pltpu.VMEM((rows, classes), BF),
            jax.ShapeDtypeStruct((LANES, LANES), F32),
            pltpu.VMEM((hid, rows), BF),
            pltpu.VMEM((hid, classes), BF),
        ],
        scratch_shapes=[
            pltpu.VMEM((halo_count, classes), BF),
            pltpu.VMEM((nodes, classes), BF),
            pltpu.VMEM((rows, nodes), BF),
            pltpu.VMEM((nodes, classes), BF),
            pltpu.VMEM((rows, classes), F32),
            pltpu.SemaphoreType.DMA((4,)),
        ],
        compiler_params=params(22),
        cost_estimate=cost(4.3, 12, 0.0005),
        name="spread",
    )(tile_cols, in_hbm(tile_weights), in_hbm(prior), halo, hslot, given, asked, in_hbm(logits), in_hbm(hidden), in_hbm(w_out_o))

    partner = [(d, d ^ 1) for d in range(128)]
    part_rows = 2 * HBLK

    def peer_part(part):
        grad = pl.pallas_call(
            partial(peer_kernel, part),
            grid_spec=pltpu.PrefetchScalarGridSpec(
                num_scalar_prefetch=1,
                grid=(2,),
                in_specs=[
                    vmem,
                    vmem,
                    vmem,
                    vmem,
                ],
                out_specs=rows_at(0, classes + feat),
            ),
            out_shape=jax.ShapeDtypeStruct((part_rows, classes + feat), BF),
            compiler_params=params(22),
            cost_estimate=cost(4.3, 9),
        )(place, w_out_o, hidden, residue, x)
        return lax.ppermute(grad, DEV, partner)

    b_spec = pl.BlockSpec((1, 256, 512), lambda i, p: (i, 0, 0))
    c_spec = pl.BlockSpec((1, 4, 64, 512), lambda i, p: (i, 0, 0, 0))
    b_shape = pltpu.HBM((2, 256, 512), BF)
    c_shape = pltpu.HBM((2, 4, 64, 512), BF)

    def own_part(part, arrived):
        return pl.pallas_call(
            partial(own_kernel, part),
            grid_spec=pltpu.PrefetchScalarGridSpec(
                num_scalar_prefetch=1,
                grid=(2,),
                in_specs=[
                    vmem,
                    vmem,
                    vmem,
                    vmem,
                    rows_at(0, classes + feat),
                    once((LANES, LANES)),
                ],
                out_specs=[rows_at(0, classes), b_spec, b_spec, c_spec, c_spec, whole((LANES, LANES))],
            ),
            out_shape=[
                pltpu.HBM((part_rows, classes), BF),
                b_shape,
                b_shape,
                c_shape,
                c_shape,
                jax.ShapeDtypeStruct((LANES, LANES), F32),
            ],
            compiler_params=params(24),
            cost_estimate=cost(4.3, 12),
        )(place, w_out_o, hidden, residue, x, arrived, errors)

    arrived = [peer_part(0), peer_part(1)]
    *first, _ = own_part(0, arrived[0])
    *second, errors_out = own_part(1, arrived[1])
    total = summed_over_chips(first, second, halves)

    back_errors = lax.all_to_all(errors_out[:, :BATCH_SLOTS], DEV, 0, 0, tiled=True)
    row_error = pl.pallas_call(
        returned_kernel,
        in_specs=[vmem] * 3,
        out_shape=jax.ShapeDtypeStruct((batch // LANES, LANES), F32),
        name="returned",
    )(back_errors, bo, brank).reshape(batch)
    return prop, row_error, total[:, 512:], total[:, :512]


def solution(mesh):
    split = Mesh(mesh.devices.reshape(128), (DEV,))
    in_specs = (
        P(DEV, None),
        P(DEV),
        P(DEV),
        P(DEV, None),
        P(DEV, None),
        P(DEV, None, None, None),
        P(DEV, None),
        P(DEV),
        P(DEV, None),
        P(DEV),
        P(),
        P(),
    )
    out_specs = (P(DEV, None), P(DEV), P(DEV, None), P(DEV, None))
    return jax.shard_map(on_device, mesh=split, in_specs=in_specs, out_specs=out_specs, check_vma=False)
```

```python
from functools import partial

import jax
import jax.numpy as jnp
from jax import lax
from jax.experimental import pallas as pl
from jax.experimental.pallas import tpu as pltpu
from jax.sharding import Mesh
from jax.sharding import PartitionSpec as P


DEV = "dev"
BF = jnp.bfloat16
F32 = jnp.float32
LANES = 128
HALO_SLOTS = 4
BATCH_SLOTS = 8
UNITS = 32
HBLK = 512


def params(mib=48, **more):
    return pltpu.CompilerParams(vmem_limit_bytes=mib * 2**20, **more)


def cost(gigaflops, mib, gigaexp=0.0):
    return pl.CostEstimate(flops=int(gigaflops * 1e9), bytes_accessed=int(mib * 2**20), transcendentals=int(gigaexp * 1e9))


def in_hbm(x):
    return pltpu.with_memory_space_constraint(x, pltpu.HBM)


def dot(left, right, dims):
    return lax.dot_general(left, right, ((dims[:1], dims[1:]), ((), ())), preferred_element_type=F32)


def ranks_of(owner_ref, blocks):
    below = lax.broadcasted_iota(jnp.int32, (LANES, LANES), 0)
    along = lax.broadcasted_iota(jnp.int32, (LANES, LANES), 1)
    rows = [owner_ref[b : b + 1, :] for b in range(blocks)]
    cols = [jnp.broadcast_to(row, (LANES, LANES)).T for row in rows]
    ranks = []
    for i in range(blocks):
        earlier = jnp.zeros((LANES, LANES), F32)
        for j in range(i + 1):
            same = cols[j] == rows[i]
            if j == i:
                same = same & (below < along)
            earlier = earlier + same.astype(F32)
        ranks.append(jnp.sum(earlier, axis=0, keepdims=True).astype(jnp.int32))
    return rows, ranks


def request_kernel(ho, hl, bo, bl, table, hslot, brank):
    device = lax.broadcasted_iota(jnp.int32, (LANES, LANES), 0)
    lane = lax.broadcasted_iota(jnp.int32, (LANES, LANES), 1)
    out = jnp.zeros((LANES, LANES), F32)
    at = 0
    for owner, local, count in ((ho, hl, HALO_SLOTS), (bo, bl, BATCH_SLOTS)):
        blocks = owner.shape[0]
        rows, ranks = ranks_of(owner, blocks)
        for s in range(count):
            total = jnp.zeros((LANES, LANES), F32)
            for i in range(blocks):
                hit = (device == rows[i]) & (ranks[i] == s)
                named = (local[i : i + 1, :] + 1).astype(F32)
                total = total + jnp.where(hit, jnp.broadcast_to(named, (LANES, LANES)), 0.0)
            out = jnp.where(lane == at, jnp.sum(total, axis=1, keepdims=True), out)
            at += 1
        for i in range(blocks):
            if owner is ho:
                hslot[i : i + 1, :] = rows[i] * HALO_SLOTS + ranks[i]
            else:
                brank[i : i + 1, :] = ranks[i]
    table[...] = out.astype(jnp.int32) - 1


def returned_kernel(errors, bo, brank, out):
    device = lax.broadcasted_iota(jnp.int32, (LANES, LANES), 0)
    for i in range(bo.shape[0]):
        total = jnp.zeros((LANES, LANES), F32)
        for s in range(BATCH_SLOTS):
            hit = (device == bo[i : i + 1, :]) & (brank[i : i + 1, :] == s)
            total = total + jnp.where(hit, errors[:, s : s + 1], 0.0)
        out[i : i + 1, :] = jnp.sum(total, axis=0, keepdims=True)


def pick_rows(table, first, count, nodes, onehot):
    node = lax.broadcasted_iota(jnp.int32, (LANES, nodes), 1)
    for s in range(count):
        wanted = table[:, first + s : first + s + 1]
        onehot[s * LANES : (s + 1) * LANES, :] = (node == wanted).astype(F32).astype(BF)


def weight_chunks(core, block):
    half = block // 4
    holder = jnp.where(half == 1, core, 1 - core)
    turn = 1 - holder
    a = (block % 4 + turn) % 4
    sources = []
    for n in range(HBLK // UNITS):
        b = (n // 4 + turn) % 4
        c = (n % 4 + turn) % 4
        sources.append(((a * 4 + b) * 4 + c) * 2 + holder)
    return sources


def fetch_chunks(core, block, far, near, sem):
    for n, source in enumerate(weight_chunks(core, block)):
        pltpu.make_async_copy(far.at[source], near.at[n], sem).start()


def first_kernel(place, table, features, w_in, w_out, x, hidden, part, onehot, acc, nodes_x, in_buf, out_buf, nodes_sem, in_sem, out_sem):
    step = pl.program_id(0)
    steps = pl.num_programs(0)
    chunks = HBLK // UNITS
    core = place[3]

    def fetch(block, slot):
        fetch_chunks(core, block, w_in, in_buf.at[slot], in_sem.at[slot])
        fetch_chunks(core, block, w_out, out_buf.at[slot], out_sem.at[slot])

    @pl.when(step == 0)
    def _():
        whole = pltpu.make_async_copy(features, nodes_x, nodes_sem)
        whole.start()
        fetch(0, 0)
        pick_rows(table, HALO_SLOTS, BATCH_SLOTS, features.shape[0], onehot)
        whole.wait()
        x[...] = dot(onehot[...], nodes_x[...], (1, 0)).astype(BF)
        acc[...] = jnp.zeros(acc.shape, F32)

    slot = step % 2

    @pl.when(step + 1 < steps)
    def _():
        fetch(step + 1, 1 - slot)

    pltpu.make_async_copy(w_in.at[pl.ds(0, chunks)], in_buf.at[slot], in_sem.at[slot]).wait()
    pltpu.make_async_copy(w_out.at[pl.ds(0, chunks)], out_buf.at[slot], out_sem.at[slot]).wait()
    h = jnp.tanh(dot(in_buf[slot].reshape(HBLK, in_buf.shape[3]), x[...], (1, 1))).astype(BF)
    hidden[...] = h
    acc[...] += dot(out_buf[slot].reshape(HBLK, out_buf.shape[3]), h, (0, 0))

    @pl.when(step == steps - 1)
    def _():
        part[...] = acc[...]


def second_kernel(
    place, x, w_in, w_out, hidden_far, part_far, prior_far, tiles_far, halo,
    hidden, w_out_near, logits, prior, tiles,
    acc, in_buf, in_sem, out_sem, sems,
):
    step = pl.program_id(0)
    steps = pl.num_programs(0)
    chunks = HBLK // UNITS
    core = place[3]
    done = hidden_far.shape[0]
    pairs = ((part_far, acc), (prior_far, prior), (tiles_far, tiles), (hidden_far, hidden.at[pl.ds(0, done)]))
    copies = [pltpu.make_async_copy(far, near, sems.at[n]) for n, (far, near) in enumerate(pairs)]

    def fetch(block, slot):
        fetch_chunks(core, block, w_in, in_buf.at[slot], in_sem.at[slot])

    def fetch_out(block):
        for n, source in enumerate(weight_chunks(core, block)):
            pltpu.make_async_copy(w_out.at[source], w_out_near.at[block * chunks + n], out_sem.at[block]).start()

    @pl.when(step == 0)
    def _():
        fetch(steps, 0)
        fetch_out(steps)
        copies[0].start()

    slot = step % 2

    @pl.when(step + 1 < steps)
    def _():
        fetch(steps + step + 1, 1 - slot)
        fetch_out(steps + step + 1)

    @pl.when(step == 0)
    def _():
        for copy in copies[1:]:
            copy.start()
        for block in range(4):
            fetch_out(block)
        copies[0].wait()

    def out_wait(block):
        here = w_out_near.at[pl.ds(block * chunks, chunks)]
        pltpu.make_async_copy(w_out.at[pl.ds(0, chunks)], here, out_sem.at[block]).wait()

    pltpu.make_async_copy(w_in.at[pl.ds(0, chunks)], in_buf.at[slot], in_sem.at[slot]).wait()
    out_wait(steps + step)
    h = jnp.tanh(dot(in_buf[slot].reshape(HBLK, in_buf.shape[3]), x[...], (1, 1))).astype(BF)
    hidden[pl.ds(pl.multiple_of(done + step * HBLK, HBLK), HBLK), :] = h
    w_out_here = w_out_near[pl.ds((steps + step) * chunks, chunks)].reshape(HBLK, w_out_near.shape[2])
    acc[...] += dot(w_out_here, h, (0, 0))

    @pl.when(step == steps - 1)
    def _():
        logits[...] = acc[...].T
        for copy in copies[1:]:
            copy.wait()
        for block in range(4):
            out_wait(block)


def spread_kernel(
    cols, weights, prior, halo, hslot, given, table, logits, prop, residue, errors, halo_tab, prop_all, onehot
):
    step = pl.program_id(0)
    per = weights.shape[0] // pl.num_programs(0)
    classes = prior.shape[1]

    @pl.when(step == 0)
    def _():
        owner = lax.broadcasted_iota(jnp.int32, (LANES, LANES), 0) * HALO_SLOTS
        for b in range(2):
            near = jnp.zeros((LANES, classes), F32)
            for k in range(HALO_SLOTS):
                pick = (owner + k == hslot[b : b + 1, :]).astype(F32).astype(BF)
                near = near + dot(pick, halo[:, k, :], (0, 0))
            halo_tab[b * LANES : (b + 1) * LANES, :] = near.astype(BF)

    for t in range(per):
        r = step * per + t
        acc = jnp.zeros((LANES, classes), F32)
        wide = jnp.zeros((LANES, LANES), F32)
        for m in range(4):
            pair = []
            for k in (2 * m, 2 * m + 1):
                wide = wide + weights[r, k].astype(F32)
                c = cols[r, k]
                if k < 6:
                    pair.append(prior[pl.ds(pl.multiple_of(c * LANES, LANES), LANES), :])
                else:
                    pair.append(halo_tab[pl.ds(pl.multiple_of((c - 16) * LANES, LANES), LANES), :])
            left = jnp.concatenate([weights[r, 2 * m], weights[r, 2 * m + 1]], axis=1)
            acc = acc + dot(left, jnp.concatenate(pair, axis=0), (1, 0))
        degree = jnp.sum(wide, axis=1, keepdims=True)
        mark = jnp.broadcast_to(given[pl.ds(r, 1), :], (LANES, LANES)).T
        lane = lax.broadcasted_iota(jnp.int32, (LANES, LANES), 1)
        seeds = jnp.concatenate([(mark == lane + g * LANES).astype(F32) for g in range(classes // LANES)], axis=1)
        mixed = (0.8 * (acc / degree) + 0.2 * seeds).astype(BF)
        prop[t * LANES : (t + 1) * LANES, :] = mixed
        prop_all[pl.ds(pl.multiple_of(r * LANES, LANES), LANES), :] = mixed

    @pl.when(step == pl.num_programs(0) - 1)
    def _():
        pick_rows(table, HALO_SLOTS, BATCH_SLOTS, prop_all.shape[0], onehot)
        lane = lax.broadcasted_iota(jnp.int32, (LANES, LANES), 1)
        out = jnp.zeros((LANES, LANES), F32)
        tall = 512
        for s in range(BATCH_SLOTS):
            at = slice(s * LANES, (s + 1) * LANES)
            if s % 4 == 0:
                picked = dot(onehot[s * LANES : s * LANES + tall, :], prop_all[...], (1, 0))
            log_z = jnp.log(picked[s % 4 * LANES : (s % 4 + 1) * LANES])
            target = log_z - jnp.mean(log_z, axis=1, keepdims=True)
            valid = table[:, HALO_SLOTS + s : HALO_SLOTS + s + 1] >= 0
            differ = jnp.where(valid, logits[at, :] - target, 0.0)
            out = jnp.where(lane == s, 0.5 * jnp.mean(differ * differ, axis=1, keepdims=True), out)
            residue[at, :] = (differ * (1.0 / 256.0)).astype(BF)
        errors[...] = out


def gradients(block, w_out, hidden, residue, x):
    at = pl.ds(pl.multiple_of(block * HBLK, HBLK), HBLK)
    h = hidden[at, :]
    wide = h.astype(F32)
    chunks = HBLK // UNITS
    w_out_here = w_out[pl.ds(block * chunks, chunks)].reshape(HBLK, w_out.shape[2])
    back = (dot(w_out_here, residue[...], (1, 1)) * (1.0 - wide * wide)).astype(BF)
    return dot(h, residue[...], (1, 0)), dot(back, x[...], (1, 0))


def peer_kernel(part, place, w_out, hidden, residue, x, grad):
    half = place[4] if part else 1 - place[4]
    out, into = gradients(2 * half + pl.program_id(0), w_out, hidden, residue, x)
    grad[:, :512] = out.astype(BF)
    grad[:, 512:] = into.astype(BF)


def own_kernel(part, place, w_out, hidden, residue, x, arrived, errors, a, send_b, keep_b, send_c, keep_c, errors_to):
    half = place[0] if part else 1 - place[0]
    out, into = gradients(4 + 2 * half + pl.program_id(0), w_out, hidden, residue, x)
    a[...] = (out + arrived[:, :512].astype(F32)).astype(BF)
    total = (into + arrived[:, 512:].astype(F32)).astype(BF)
    left = total[:, :512].reshape(2, 256, 512)
    right = total[:, 512:].reshape(4, 2, 64, 512)

    for half in range(2):

        @pl.when(place[1] == half)
        def _():
            keep_b[0] = left[half]
            send_b[0] = left[1 - half]

        @pl.when(place[2] == half)
        def _():
            keep_c[0] = right[:, half]
            send_c[0] = right[:, 1 - half]

    errors_to[...] = errors[...]


def pairing(level, dims):
    flip = 3 if level == 1 else 1
    pairs = []
    for source in range(128):
        core = source % 2
        spot = [source // 32, (source // 8) % 4, (source // 2) % 4]
        for d in dims:
            shifted = (spot[d] - (1 - core)) % 4
            spot[d] = ((shifted ^ flip) + (1 - core)) % 4
        pairs.append((source, ((spot[0] * 4 + spot[1]) * 4 + spot[2]) * 2 + core))
    return pairs


def exchange(x, level, dims):
    return lax.ppermute(x, DEV, pairing(level, dims))


def corners():
    groups = []
    for core in range(2):
        for high in range(8):
            group = []
            for low in range(8):
                shifted = [2 * ((high >> (2 - d)) & 1) + ((low >> (2 - d)) & 1) for d in range(3)]
                a, b, c = ((v + 1 - core) % 4 for v in shifted)
                group.append(((a * 4 + b) * 4 + c) * 2 + core)
            groups.append(group)
    return groups


def deal_kernel(k0, r0, k1, r1, k2, r2, pieces):
    for m in range(8):
        at = (m >> 2, (m >> 1) & 1, m & 1)
        for j, (k, r) in enumerate(((k0, r0), (k1, r1), (k2, r2))):
            piece = k[at].astype(F32) + r[at].astype(F32)
            pieces[m, :, j * 512 : (j + 1) * 512] = piece.astype(BF)


def finish_kernel(dealt, into, out):
    total = jnp.sum(dealt[...].astype(F32), axis=0)
    out[...] = total[:, :512]
    into[...] = total[:, 512:]


def summed_over_chips(first, second, halves):
    shape_a, shape_b, shape_c = (2, 4, 4, UNITS, 512), (2, 2, 4, UNITS, 512), (2, 4, 2, UNITS, 512)
    send_a, send_b1, keep_b1, send_c1, keep_c1 = first
    keep_a, send_b2, keep_b2, send_c2, keep_c2 = second
    got_c1 = exchange(send_c1, 1, (2,)).reshape(shape_c)
    got_b1 = exchange(send_b1, 1, (1,)).reshape(shape_b)
    got_a = exchange(send_a, 1, (0,)).reshape(shape_a)
    got_c2 = exchange(send_c2, 1, (2,)).reshape(shape_c)
    got_b2 = exchange(send_b2, 1, (1,)).reshape(shape_b)
    keep_a = keep_a.reshape(shape_a)
    keep_b1, keep_b2 = keep_b1.reshape(shape_b), keep_b2.reshape(shape_b)
    keep_c1, keep_c2 = keep_c1.reshape(shape_c), keep_c2.reshape(shape_c)

    def added(kept, got, dim=None, half=None):
        if dim is not None:
            kept, got = (lax.dynamic_slice_in_dim(v, 2 * half, 2, dim) for v in (kept, got))
        return kept.astype(F32) + got.astype(F32)

    def sent(value, dim):
        return exchange(value.astype(BF), 1, (dim,))

    _, hb, hc = halves
    c1_send = added(keep_c1, got_c1, 1, 1 - hb)
    c1_got = sent(c1_send, 1)
    b_send = added(keep_b1, got_b1)
    b_got = sent(b_send, 0)
    a_send = added(keep_a, got_a, 2, 1 - hc)
    a_got = sent(a_send, 2)
    c2_send = added(keep_c2, got_c2, 1, 1 - hb).astype(BF)
    c2_got = sent(c2_send, 1)
    b = added(keep_b2, got_b2).astype(BF)
    a = added(keep_a, got_a, 2, hc).astype(BF)
    c1 = added(keep_c1, got_c1, 1, hb).astype(BF)
    c2 = added(keep_c2, got_c2, 1, hb).astype(BF)
    b_last = sent(added(b, b_got, 2, 1 - hc), 2)
    a_last = sent(added(a, a_got, 1, 1 - hb), 1)
    c_last = sent(added(c1, c1_got), 0)
    b = added(b, b_got, 2, hc)
    a = added(a, a_got, 1, hb)
    c = added(c2, c2_got)
    pieces = pl.pallas_call(
        deal_kernel,
        in_specs=[pl.BlockSpec(memory_space=pltpu.VMEM)] * 6,
        out_specs=pl.BlockSpec(memory_space=pltpu.VMEM),
        out_shape=jax.ShapeDtypeStruct((8, UNITS, 1536), BF),
        compiler_params=params(16),
        name="deal",
    )(a, a_last, b, b_last, c, c_last)
    dealt = lax.all_to_all(pieces, DEV, 0, 0, axis_index_groups=corners(), tiled=True)
    return pl.pallas_call(
        finish_kernel,
        in_specs=[pl.BlockSpec(memory_space=pltpu.VMEM)],
        out_shape=[jax.ShapeDtypeStruct((UNITS, 1024), F32), jax.ShapeDtypeStruct((UNITS, 512), F32)],
        name="finish",
    )(dealt)


def on_device(prior, label_class, labeled, features, tile_cols, tile_weights, halo_owner, halo_local, batch_owner, batch_local, w_in, w_out):
    nodes, classes = prior.shape
    feat = features.shape[1]
    hid = w_in.shape[0]
    halo_count = halo_local.shape[0]
    batch = batch_local.shape[0]
    rows = BATCH_SLOTS * LANES
    me = lax.axis_index(DEV)
    core = me % 2
    chip = (me // 32, (me // 8) % 4, (me // 2) % 4)
    spots = [(s + 3 + core) % 4 for s in chip]
    halves = [s // 2 for s in spots]
    peer_half = (chip[0] + 4 - core) % 4 // 2
    place = jnp.stack([*halves, core, peer_half]).astype(jnp.int32)
    vmem = pl.BlockSpec(memory_space=pltpu.VMEM)
    smem = pl.BlockSpec(memory_space=pltpu.SMEM)
    hbm = pl.BlockSpec(memory_space=pl.ANY)
    i32 = jnp.int32

    bo = batch_owner.reshape(batch // LANES, LANES)
    table, hslot, brank = pl.pallas_call(
        request_kernel,
        in_specs=[vmem] * 4,
        out_shape=[
            jax.ShapeDtypeStruct((LANES, LANES), i32),
            jax.ShapeDtypeStruct((halo_count // LANES, LANES), i32),
            jax.ShapeDtypeStruct((batch // LANES, LANES), i32),
        ],
        name="request",
    )(
        halo_owner.reshape(halo_count // LANES, LANES),
        halo_local.reshape(halo_count // LANES, LANES),
        bo,
        batch_local.reshape(batch // LANES, LANES),
    )
    asked = lax.all_to_all(table[:, : HALO_SLOTS + BATCH_SLOTS], DEV, 0, 0, tiled=True)

    served = prior[jnp.maximum(asked[:, :HALO_SLOTS], 0)]
    halo = lax.all_to_all(served, DEV, 0, 0, tiled=True)

    def whole(shape):
        return pl.BlockSpec(shape, lambda i, *_: (0,) * len(shape))

    def once(shape):
        return pl.BlockSpec(shape, lambda i, *_: (0,) * len(shape), pipeline_mode=pl.Buffered(1))

    def rows_at(offset, width):
        return pl.BlockSpec((HBLK, width), lambda i, *_: (i + offset, 0))

    slots = HALO_SLOTS + BATCH_SLOTS
    chunks = HBLK // UNITS
    steps = hid // HBLK // 2
    w_in = w_in.reshape(128, UNITS, feat)
    w_out = w_out.reshape(128, UNITS, classes)
    x, hidden_first, part = pl.pallas_call(
        first_kernel,
        grid=(steps,),
        in_specs=[smem, once((LANES, slots)), hbm, hbm, hbm],
        out_specs=[vmem, rows_at(0, rows), whole((classes, rows))],
        out_shape=[pltpu.VMEM((rows, feat), BF), pltpu.HBM((hid // 2, rows), BF), pltpu.HBM((classes, rows), F32)],
        scratch_shapes=[
            pltpu.VMEM((rows, nodes), BF),
            pltpu.VMEM((classes, rows), F32),
            pltpu.VMEM((nodes, feat), BF),
            pltpu.VMEM((2, chunks, UNITS, feat), BF),
            pltpu.VMEM((2, chunks, UNITS, classes), BF),
            pltpu.SemaphoreType.DMA,
            pltpu.SemaphoreType.DMA((2,)),
            pltpu.SemaphoreType.DMA((2,)),
        ],
        compiler_params=params(32),
        cost_estimate=cost(10.7, 16, 0.0021),
        name="first",
    )(place, asked, in_hbm(features), in_hbm(w_in), in_hbm(w_out))
    hidden, w_out_o, logits, prior_near, tiles_near = pl.pallas_call(
        second_kernel,
        grid=(steps,),
        in_specs=[smem, vmem, hbm, hbm, hbm, hbm, hbm, hbm, hbm],
        out_specs=[vmem] * 5,
        out_shape=[
            pltpu.VMEM((hid, rows), BF),
            pltpu.VMEM((128, UNITS, classes), BF),
            pltpu.VMEM((rows, classes), F32),
            pltpu.VMEM((nodes, classes), BF),
            pltpu.VMEM(tile_weights.shape, BF),
        ],
        scratch_shapes=[
            pltpu.VMEM((classes, rows), F32),
            pltpu.VMEM((2, chunks, UNITS, feat), BF),
            pltpu.SemaphoreType.DMA((2,)),
            pltpu.SemaphoreType.DMA((8,)),
            pltpu.SemaphoreType.DMA((4,)),
        ],
        compiler_params=params(16),
        cost_estimate=cost(6.5, 22, 0.0021),
        name="second",
    )(
        place,
        x,
        in_hbm(w_in),
        in_hbm(w_out),
        in_hbm(hidden_first),
        in_hbm(part),
        in_hbm(prior),
        in_hbm(tile_weights),
        halo,
    )

    row_tiles = tile_weights.shape[0]
    per = 2
    given = jnp.where(labeled == 1, label_class, -1).reshape(row_tiles, LANES)
    prop, residue, errors = pl.pallas_call(
        spread_kernel,
        grid=(row_tiles // per,),
        in_specs=[
            smem,
            vmem,
            vmem,
            vmem,
            once((halo_count // LANES, LANES)),
            once((row_tiles, LANES)),
            once((LANES, slots)),
            vmem,
        ],
        out_specs=[
            pl.BlockSpec((per * LANES, classes), lambda i: (i, 0)),
            vmem,
            whole((LANES, LANES)),
        ],
        out_shape=[
            jax.ShapeDtypeStruct((nodes, classes), BF),
            pltpu.VMEM((rows, classes), BF),
            jax.ShapeDtypeStruct((LANES, LANES), F32),
        ],
        scratch_shapes=[
            pltpu.VMEM((halo_count, classes), BF),
            pltpu.VMEM((nodes, classes), BF),
            pltpu.VMEM((rows, nodes), BF),
        ],
        compiler_params=params(22),
        cost_estimate=cost(4.3, 12, 0.0005),
        name="spread",
    )(tile_cols, tiles_near, prior_near, halo, hslot, given, asked, logits)

    partner = [(d, d ^ 1) for d in range(128)]
    part_rows = 2 * HBLK

    def peer_part(part):
        grad = pl.pallas_call(
            partial(peer_kernel, part),
            grid_spec=pltpu.PrefetchScalarGridSpec(
                num_scalar_prefetch=1,
                grid=(2,),
                in_specs=[
                    vmem,
                    vmem,
                    vmem,
                    vmem,
                ],
                out_specs=rows_at(0, classes + feat),
            ),
            out_shape=jax.ShapeDtypeStruct((part_rows, classes + feat), BF),
            compiler_params=params(22),
            cost_estimate=cost(4.3, 9),
        )(place, w_out_o, hidden, residue, x)
        return lax.ppermute(grad, DEV, partner)

    b_spec = pl.BlockSpec((1, 256, 512), lambda i, p: (i, 0, 0))
    c_spec = pl.BlockSpec((1, 4, 64, 512), lambda i, p: (i, 0, 0, 0))
    b_shape = pltpu.HBM((2, 256, 512), BF)
    c_shape = pltpu.HBM((2, 4, 64, 512), BF)

    def own_part(part, arrived):
        return pl.pallas_call(
            partial(own_kernel, part),
            grid_spec=pltpu.PrefetchScalarGridSpec(
                num_scalar_prefetch=1,
                grid=(2,),
                in_specs=[
                    vmem,
                    vmem,
                    vmem,
                    vmem,
                    rows_at(0, classes + feat),
                    once((LANES, LANES)),
                ],
                out_specs=[rows_at(0, classes), b_spec, b_spec, c_spec, c_spec, whole((LANES, LANES))],
            ),
            out_shape=[
                pltpu.HBM((part_rows, classes), BF),
                b_shape,
                b_shape,
                c_shape,
                c_shape,
                jax.ShapeDtypeStruct((LANES, LANES), F32),
            ],
            compiler_params=params(24),
            cost_estimate=cost(4.3, 12),
        )(place, w_out_o, hidden, residue, x, arrived, errors)

    arrived = [peer_part(0), peer_part(1)]
    *first, _ = own_part(0, arrived[0])
    *second, errors_out = own_part(1, arrived[1])
    grad_in, grad_out = summed_over_chips(first, second, halves)

    back_errors = lax.all_to_all(errors_out[:, :BATCH_SLOTS], DEV, 0, 0, tiled=True)
    row_error = pl.pallas_call(
        returned_kernel,
        in_specs=[vmem] * 3,
        out_shape=jax.ShapeDtypeStruct((batch // LANES, LANES), F32),
        name="returned",
    )(back_errors, bo, brank).reshape(batch)
    return prop, row_error, grad_in, grad_out


def solution(mesh):
    split = Mesh(mesh.devices.reshape(128), (DEV,))
    in_specs = (
        P(DEV, None),
        P(DEV),
        P(DEV),
        P(DEV, None),
        P(DEV, None),
        P(DEV, None, None, None),
        P(DEV, None),
        P(DEV),
        P(DEV, None),
        P(DEV),
        P(),
        P(),
    )
    out_specs = (P(DEV, None), P(DEV), P(DEV, None), P(DEV, None))
    return jax.shard_map(on_device, mesh=split, in_specs=in_specs, out_specs=out_specs, check_vma=False)
```

```python
from functools import partial

import jax
import jax.numpy as jnp
from jax import lax
from jax.experimental import pallas as pl
from jax.experimental.pallas import tpu as pltpu
from jax.sharding import Mesh
from jax.sharding import PartitionSpec as P


DEV = "dev"
BF = jnp.bfloat16
F32 = jnp.float32
LANES = 128
HALO_SLOTS = 4
BATCH_SLOTS = 8
UNITS = 32
HBLK = 512


def params(mib=48, **more):
    return pltpu.CompilerParams(vmem_limit_bytes=mib * 2**20, **more)


def cost(gigaflops, mib, gigaexp=0.0):
    return pl.CostEstimate(flops=int(gigaflops * 1e9), bytes_accessed=int(mib * 2**20), transcendentals=int(gigaexp * 1e9))


def in_hbm(x):
    return pltpu.with_memory_space_constraint(x, pltpu.HBM)


def dot(left, right, dims):
    return lax.dot_general(left, right, ((dims[:1], dims[1:]), ((), ())), preferred_element_type=F32)


def ranks_of(owner_ref, blocks):
    below = lax.broadcasted_iota(jnp.int32, (LANES, LANES), 0)
    along = lax.broadcasted_iota(jnp.int32, (LANES, LANES), 1)
    rows = [owner_ref[b : b + 1, :] for b in range(blocks)]
    cols = [jnp.broadcast_to(row, (LANES, LANES)).T for row in rows]
    ranks = []
    for i in range(blocks):
        earlier = jnp.zeros((LANES, LANES), F32)
        for j in range(i + 1):
            same = cols[j] == rows[i]
            if j == i:
                same = same & (below < along)
            earlier = earlier + same.astype(F32)
        ranks.append(jnp.sum(earlier, axis=0, keepdims=True).astype(jnp.int32))
    return rows, ranks


def request_kernel(ho, hl, bo, bl, table, hslot, brank):
    device = lax.broadcasted_iota(jnp.int32, (LANES, LANES), 0)
    lane = lax.broadcasted_iota(jnp.int32, (LANES, LANES), 1)
    out = jnp.zeros((LANES, LANES), F32)
    at = 0
    for owner, local, count in ((ho, hl, HALO_SLOTS), (bo, bl, BATCH_SLOTS)):
        blocks = owner.shape[0]
        rows, ranks = ranks_of(owner, blocks)
        for s in range(count):
            total = jnp.zeros((LANES, LANES), F32)
            for i in range(blocks):
                hit = (device == rows[i]) & (ranks[i] == s)
                named = (local[i : i + 1, :] + 1).astype(F32)
                total = total + jnp.where(hit, jnp.broadcast_to(named, (LANES, LANES)), 0.0)
            out = jnp.where(lane == at, jnp.sum(total, axis=1, keepdims=True), out)
            at += 1
        for i in range(blocks):
            if owner is ho:
                hslot[i : i + 1, :] = rows[i] * HALO_SLOTS + ranks[i]
            else:
                brank[i : i + 1, :] = ranks[i]
    table[...] = out.astype(jnp.int32) - 1


def device_at(core, high, low):
    device = 0
    for d in (2, 1, 0):
        spot = (2 * ((high >> d) & 1) + ((low >> d) & 1) + 1 - core) % 4
        device = device * 4 + spot
    return device * 2 + core


def pick_rows(table, first, count, nodes, onehot):
    node = lax.broadcasted_iota(jnp.int32, (LANES, nodes), 1)
    for s in range(count):
        wanted = table[:, first + s : first + s + 1]
        onehot[s * LANES : (s + 1) * LANES, :] = (node == wanted).astype(F32).astype(BF)


def weight_chunks(core, block):
    half = block // 4
    holder = jnp.where(half == 1, core, 1 - core)
    turn = 1 - holder
    a = (block % 4 + turn) % 4
    sources = []
    for n in range(HBLK // UNITS):
        b = (n // 4 + turn) % 4
        c = (n % 4 + turn) % 4
        sources.append(((a * 4 + b) * 4 + c) * 2 + holder)
    return sources


def fetch_chunks(core, block, far, near, sem):
    for n, source in enumerate(weight_chunks(core, block)):
        pltpu.make_async_copy(far.at[source], near.at[n], sem).start()


def first_kernel(place, table, features, w_in, w_out, x, hidden, part, onehot, acc, nodes_x, in_buf, out_buf, nodes_sem, in_sem, out_sem):
    step = pl.program_id(0)
    steps = pl.num_programs(0)
    chunks = HBLK // UNITS
    core = place[3]

    def fetch(block, slot):
        fetch_chunks(core, block, w_in, in_buf.at[slot], in_sem.at[slot])
        fetch_chunks(core, block, w_out, out_buf.at[slot], out_sem.at[slot])

    @pl.when(step == 0)
    def _():
        whole = pltpu.make_async_copy(features, nodes_x, nodes_sem)
        whole.start()
        fetch(0, 0)
        pick_rows(table, HALO_SLOTS, BATCH_SLOTS, features.shape[0], onehot)
        whole.wait()
        x[...] = dot(onehot[...], nodes_x[...], (1, 0)).astype(BF)
        acc[...] = jnp.zeros(acc.shape, F32)

    slot = step % 2

    @pl.when(step + 1 < steps)
    def _():
        fetch(step + 1, 1 - slot)

    pltpu.make_async_copy(w_in.at[pl.ds(0, chunks)], in_buf.at[slot], in_sem.at[slot]).wait()
    pltpu.make_async_copy(w_out.at[pl.ds(0, chunks)], out_buf.at[slot], out_sem.at[slot]).wait()
    h = jnp.tanh(dot(in_buf[slot].reshape(HBLK, in_buf.shape[3]), x[...], (1, 1))).astype(BF)
    hidden[...] = h
    acc[...] += dot(out_buf[slot].reshape(HBLK, out_buf.shape[3]), h, (0, 0))

    @pl.when(step == steps - 1)
    def _():
        part[...] = acc[...]


def second_kernel(
    place, x, w_in, w_out, hidden_far, part_far, prior_far, tiles_far, halo,
    hidden, w_out_near, logits, prior, tiles,
    acc, in_buf, in_sem, out_sem, sems,
):
    step = pl.program_id(0)
    steps = pl.num_programs(0)
    chunks = HBLK // UNITS
    core = place[3]
    done = hidden_far.shape[0]
    pairs = ((part_far, acc), (prior_far, prior), (tiles_far, tiles), (hidden_far, hidden.at[pl.ds(0, done)]))
    copies = [pltpu.make_async_copy(far, near, sems.at[n]) for n, (far, near) in enumerate(pairs)]

    def fetch(block, slot):
        fetch_chunks(core, block, w_in, in_buf.at[slot], in_sem.at[slot])

    def fetch_out(block):
        for n, source in enumerate(weight_chunks(core, block)):
            pltpu.make_async_copy(w_out.at[source], w_out_near.at[block * chunks + n], out_sem.at[block]).start()

    @pl.when(step == 0)
    def _():
        fetch(steps, 0)
        fetch_out(steps)
        copies[0].start()

    slot = step % 2

    @pl.when(step + 1 < steps)
    def _():
        fetch(steps + step + 1, 1 - slot)
        fetch_out(steps + step + 1)

    @pl.when(step == 0)
    def _():
        for copy in copies[1:]:
            copy.start()
        for block in range(4):
            fetch_out(block)
        copies[0].wait()

    def out_wait(block):
        here = w_out_near.at[pl.ds(block * chunks, chunks)]
        pltpu.make_async_copy(w_out.at[pl.ds(0, chunks)], here, out_sem.at[block]).wait()

    pltpu.make_async_copy(w_in.at[pl.ds(0, chunks)], in_buf.at[slot], in_sem.at[slot]).wait()
    out_wait(steps + step)
    h = jnp.tanh(dot(in_buf[slot].reshape(HBLK, in_buf.shape[3]), x[...], (1, 1))).astype(BF)
    hidden[pl.ds(pl.multiple_of(done + step * HBLK, HBLK), HBLK), :] = h
    w_out_here = w_out_near[pl.ds((steps + step) * chunks, chunks)].reshape(HBLK, w_out_near.shape[2])
    acc[...] += dot(w_out_here, h, (0, 0))

    @pl.when(step == steps - 1)
    def _():
        logits[...] = acc[...].T
        for copy in copies[1:]:
            copy.wait()
        for block in range(4):
            out_wait(block)


def spread_kernel(
    cols, weights, prior, halo, hslot, given, table, logits, prop, residue, errors, halo_tab, prop_all, onehot
):
    step = pl.program_id(0)
    per = weights.shape[0] // pl.num_programs(0)
    classes = prior.shape[1]

    @pl.when(step == 0)
    def _():
        owner = lax.broadcasted_iota(jnp.int32, (LANES, LANES), 0) * HALO_SLOTS
        for b in range(2):
            near = jnp.zeros((LANES, classes), F32)
            for k in range(HALO_SLOTS):
                pick = (owner + k == hslot[b : b + 1, :]).astype(F32).astype(BF)
                near = near + dot(pick, halo[:, k, :], (0, 0))
            halo_tab[b * LANES : (b + 1) * LANES, :] = near.astype(BF)

    for t in range(per):
        r = step * per + t
        acc = jnp.zeros((LANES, classes), F32)
        wide = jnp.zeros((LANES, LANES), F32)
        for m in range(4):
            pair = []
            for k in (2 * m, 2 * m + 1):
                wide = wide + weights[r, k].astype(F32)
                c = cols[r, k]
                if k < 6:
                    pair.append(prior[pl.ds(pl.multiple_of(c * LANES, LANES), LANES), :])
                else:
                    pair.append(halo_tab[pl.ds(pl.multiple_of((c - 16) * LANES, LANES), LANES), :])
            left = jnp.concatenate([weights[r, 2 * m], weights[r, 2 * m + 1]], axis=1)
            acc = acc + dot(left, jnp.concatenate(pair, axis=0), (1, 0))
        degree = jnp.sum(wide, axis=1, keepdims=True)
        mark = jnp.broadcast_to(given[pl.ds(r, 1), :], (LANES, LANES)).T
        lane = lax.broadcasted_iota(jnp.int32, (LANES, LANES), 1)
        seeds = jnp.concatenate([(mark == lane + g * LANES).astype(F32) for g in range(classes // LANES)], axis=1)
        mixed = (0.8 * (acc / degree) + 0.2 * seeds).astype(BF)
        prop[t * LANES : (t + 1) * LANES, :] = mixed
        prop_all[pl.ds(pl.multiple_of(r * LANES, LANES), LANES), :] = mixed

    @pl.when(step == pl.num_programs(0) - 1)
    def _():
        pick_rows(table, HALO_SLOTS, BATCH_SLOTS, prop_all.shape[0], onehot)
        lane = lax.broadcasted_iota(jnp.int32, (LANES, LANES), 1)
        out = jnp.zeros((LANES, LANES), F32)
        tall = 512
        for s in range(BATCH_SLOTS):
            at = slice(s * LANES, (s + 1) * LANES)
            if s % 4 == 0:
                picked = dot(onehot[s * LANES : s * LANES + tall, :], prop_all[...], (1, 0))
            log_z = jnp.log(picked[s % 4 * LANES : (s % 4 + 1) * LANES])
            target = log_z - jnp.mean(log_z, axis=1, keepdims=True)
            valid = table[:, HALO_SLOTS + s : HALO_SLOTS + s + 1] >= 0
            differ = jnp.where(valid, logits[at, :] - target, 0.0)
            out = jnp.where(lane == s, 0.5 * jnp.mean(differ * differ, axis=1, keepdims=True), out)
            residue[at, :] = (differ * (1.0 / 256.0)).astype(BF)
        errors[...] = out


def gradients(block, w_out, hidden, residue, x):
    at = pl.ds(pl.multiple_of(block * HBLK, HBLK), HBLK)
    h = hidden[at, :]
    wide = h.astype(F32)
    chunks = HBLK // UNITS
    w_out_here = w_out[pl.ds(block * chunks, chunks)].reshape(HBLK, w_out.shape[2])
    back = (dot(w_out_here, residue[...], (1, 1)) * (1.0 - wide * wide)).astype(BF)
    return dot(h, residue[...], (1, 0)), dot(back, x[...], (1, 0))


def peer_kernel(part, place, w_out, hidden, residue, x, grad):
    half = place[4] if part else 1 - place[4]
    out, into = gradients(2 * half + pl.program_id(0), w_out, hidden, residue, x)
    grad[:, :512] = out.astype(BF)
    grad[:, 512:] = into.astype(BF)


def own_kernel(part, place, w_out, hidden, residue, x, arrived, errors, a, send_b, keep_b, send_c, keep_c, errors_to):
    half = place[0] if part else 1 - place[0]
    out, into = gradients(4 + 2 * half + pl.program_id(0), w_out, hidden, residue, x)
    a[...] = (out + arrived[:, :512].astype(F32)).astype(BF)
    total = (into + arrived[:, 512:].astype(F32)).astype(BF)
    left = total[:, :512].reshape(2, 256, 512)
    right = total[:, 512:].reshape(4, 2, 64, 512)

    for half in range(2):

        @pl.when(place[1] == half)
        def _():
            keep_b[0] = left[half]
            send_b[0] = left[1 - half]

        @pl.when(place[2] == half)
        def _():
            keep_c[0] = right[:, half]
            send_c[0] = right[:, 1 - half]

    if not part:
        errors_to[...] = errors[...]
        return

    @pl.when(pl.program_id(0) == 0)
    def _():
        row = lax.broadcasted_iota(jnp.int32, (LANES, LANES), 0)
        device = lax.broadcasted_iota(jnp.int32, (LANES, LANES), 1)
        pick = (device_at(row >> 6, (row >> 3) & 7, row & 7) == device).astype(F32).astype(BF)
        moved = [dot(pick, third, (1, 0)) for third in thirds(errors[...])]
        errors_to[...] = moved[0] + moved[1] + moved[2]


def pairing(level, dims):
    flip = 3 if level == 1 else 1
    pairs = []
    for source in range(128):
        core = source % 2
        spot = [source // 32, (source // 8) % 4, (source // 2) % 4]
        for d in dims:
            shifted = (spot[d] - (1 - core)) % 4
            spot[d] = ((shifted ^ flip) + (1 - core)) % 4
        pairs.append((source, ((spot[0] * 4 + spot[1]) * 4 + spot[2]) * 2 + core))
    return pairs


def exchange(x, level, dims):
    return lax.ppermute(x, DEV, pairing(level, dims))


def corners():
    return [[device_at(core, high, low) for low in range(8)] for core in range(2) for high in range(8)]


def across():
    return [[device_at(core, high, low) for core in range(2) for high in range(8)] for low in range(8)]


def thirds(value):
    high = value.astype(BF)
    rest = value - high.astype(F32)
    middle = rest.astype(BF)
    return high, middle, (rest - middle.astype(F32)).astype(BF)


def deal_kernel(k0, r0, k1, r1, k2, r2, errors, pieces):
    for m in range(8):
        at = (m >> 2, (m >> 1) & 1, m & 1)
        for j, (k, r) in enumerate(((k0, r0), (k1, r1), (k2, r2))):
            piece = k[at].astype(F32) + r[at].astype(F32)
            pieces[m, :UNITS, j * 512 : (j + 1) * 512] = piece.astype(BF)
        for n, third in enumerate(thirds(errors[:, m, :])):
            pieces[m, UNITS:, n * LANES : n * LANES + BATCH_SLOTS] = third


def finish_kernel(dealt, bo, brank, into, out, row_error):
    total = jnp.sum(dealt[:, :UNITS, :].astype(F32), axis=0)
    out[...] = total[:, :512]
    into[...] = total[:, 512:]
    mine = []
    for m in range(8):
        parts = [dealt[m, UNITS:, n * LANES : n * LANES + BATCH_SLOTS].astype(F32) for n in range(3)]
        mine.append(parts[0] + parts[1] + parts[2])
    errors = jnp.concatenate(mine, axis=0)
    row = lax.broadcasted_iota(jnp.int32, (LANES, LANES), 0)
    device = device_at((row >> 3) & 1, row & 7, row >> 4)
    for i in range(bo.shape[0]):
        found = jnp.zeros((LANES, LANES), F32)
        for s in range(BATCH_SLOTS):
            hit = (device == bo[i : i + 1, :]) & (brank[i : i + 1, :] == s)
            found = found + jnp.where(hit, errors[:, s : s + 1], 0.0)
        row_error[i : i + 1, :] = jnp.sum(found, axis=0, keepdims=True)


def summed_over_chips(first, second, halves, errors, bo, brank):
    shape_a, shape_b, shape_c = (2, 4, 4, UNITS, 512), (2, 2, 4, UNITS, 512), (2, 4, 2, UNITS, 512)
    send_a, send_b1, keep_b1, send_c1, keep_c1 = first
    keep_a, send_b2, keep_b2, send_c2, keep_c2 = second
    got_c1 = exchange(send_c1, 1, (2,)).reshape(shape_c)
    got_b1 = exchange(send_b1, 1, (1,)).reshape(shape_b)
    got_a = exchange(send_a, 1, (0,)).reshape(shape_a)
    got_c2 = exchange(send_c2, 1, (2,)).reshape(shape_c)
    got_b2 = exchange(send_b2, 1, (1,)).reshape(shape_b)
    keep_a = keep_a.reshape(shape_a)
    keep_b1, keep_b2 = keep_b1.reshape(shape_b), keep_b2.reshape(shape_b)
    keep_c1, keep_c2 = keep_c1.reshape(shape_c), keep_c2.reshape(shape_c)

    def added(kept, got, dim=None, half=None):
        if dim is not None:
            kept, got = (lax.dynamic_slice_in_dim(v, 2 * half, 2, dim) for v in (kept, got))
        return kept.astype(F32) + got.astype(F32)

    def sent(value, dim):
        return exchange(value.astype(BF), 1, (dim,))

    _, hb, hc = halves
    arrived = lax.all_to_all(errors, DEV, 0, 0, axis_index_groups=across(), tiled=True)
    c1_send = added(keep_c1, got_c1, 1, 1 - hb)
    c1_got = sent(c1_send, 1)
    b_send = added(keep_b1, got_b1)
    b_got = sent(b_send, 0)
    a_send = added(keep_a, got_a, 2, 1 - hc)
    a_got = sent(a_send, 2)
    c2_send = added(keep_c2, got_c2, 1, 1 - hb).astype(BF)
    c2_got = sent(c2_send, 1)
    b = added(keep_b2, got_b2).astype(BF)
    a = added(keep_a, got_a, 2, hc).astype(BF)
    c1 = added(keep_c1, got_c1, 1, hb).astype(BF)
    c2 = added(keep_c2, got_c2, 1, hb).astype(BF)
    b_last = sent(added(b, b_got, 2, 1 - hc), 2)
    a_last = sent(added(a, a_got, 1, 1 - hb), 1)
    c_last = sent(added(c1, c1_got), 0)
    b = added(b, b_got, 2, hc)
    a = added(a, a_got, 1, hb)
    c = added(c2, c2_got)
    pieces = pl.pallas_call(
        deal_kernel,
        in_specs=[pl.BlockSpec(memory_space=pltpu.VMEM)] * 7,
        out_specs=pl.BlockSpec(memory_space=pltpu.VMEM),
        out_shape=jax.ShapeDtypeStruct((8, UNITS + 16, 1536), BF),
        compiler_params=params(16),
        name="deal",
    )(a, a_last, b, b_last, c, c_last, arrived.reshape(16, 8, BATCH_SLOTS))
    dealt = lax.all_to_all(pieces, DEV, 0, 0, axis_index_groups=corners(), tiled=True)
    return pl.pallas_call(
        finish_kernel,
        in_specs=[pl.BlockSpec(memory_space=pltpu.VMEM)] * 3,
        out_shape=[
            jax.ShapeDtypeStruct((UNITS, 1024), F32),
            jax.ShapeDtypeStruct((UNITS, 512), F32),
            jax.ShapeDtypeStruct(bo.shape, F32),
        ],
        name="finish",
    )(dealt, bo, brank)


def on_device(prior, label_class, labeled, features, tile_cols, tile_weights, halo_owner, halo_local, batch_owner, batch_local, w_in, w_out):
    nodes, classes = prior.shape
    feat = features.shape[1]
    hid = w_in.shape[0]
    halo_count = halo_local.shape[0]
    batch = batch_local.shape[0]
    rows = BATCH_SLOTS * LANES
    me = lax.axis_index(DEV)
    core = me % 2
    chip = (me // 32, (me // 8) % 4, (me // 2) % 4)
    spots = [(s + 3 + core) % 4 for s in chip]
    halves = [s // 2 for s in spots]
    peer_half = (chip[0] + 4 - core) % 4 // 2
    place = jnp.stack([*halves, core, peer_half]).astype(jnp.int32)
    vmem = pl.BlockSpec(memory_space=pltpu.VMEM)
    smem = pl.BlockSpec(memory_space=pltpu.SMEM)
    hbm = pl.BlockSpec(memory_space=pl.ANY)
    i32 = jnp.int32

    bo = batch_owner.reshape(batch // LANES, LANES)
    table, hslot, brank = pl.pallas_call(
        request_kernel,
        in_specs=[vmem] * 4,
        out_shape=[
            jax.ShapeDtypeStruct((LANES, LANES), i32),
            jax.ShapeDtypeStruct((halo_count // LANES, LANES), i32),
            jax.ShapeDtypeStruct((batch // LANES, LANES), i32),
        ],
        name="request",
    )(
        halo_owner.reshape(halo_count // LANES, LANES),
        halo_local.reshape(halo_count // LANES, LANES),
        bo,
        batch_local.reshape(batch // LANES, LANES),
    )
    asked = lax.all_to_all(table[:, : HALO_SLOTS + BATCH_SLOTS], DEV, 0, 0, tiled=True)

    served = prior[jnp.maximum(asked[:, :HALO_SLOTS], 0)]
    halo = lax.all_to_all(served, DEV, 0, 0, tiled=True)

    def whole(shape):
        return pl.BlockSpec(shape, lambda i, *_: (0,) * len(shape))

    def once(shape):
        return pl.BlockSpec(shape, lambda i, *_: (0,) * len(shape), pipeline_mode=pl.Buffered(1))

    def rows_at(offset, width):
        return pl.BlockSpec((HBLK, width), lambda i, *_: (i + offset, 0))

    slots = HALO_SLOTS + BATCH_SLOTS
    chunks = HBLK // UNITS
    steps = hid // HBLK // 2
    w_in = w_in.reshape(128, UNITS, feat)
    w_out = w_out.reshape(128, UNITS, classes)
    x, hidden_first, part = pl.pallas_call(
        first_kernel,
        grid=(steps,),
        in_specs=[smem, once((LANES, slots)), hbm, hbm, hbm],
        out_specs=[vmem, rows_at(0, rows), whole((classes, rows))],
        out_shape=[pltpu.VMEM((rows, feat), BF), pltpu.HBM((hid // 2, rows), BF), pltpu.HBM((classes, rows), F32)],
        scratch_shapes=[
            pltpu.VMEM((rows, nodes), BF),
            pltpu.VMEM((classes, rows), F32),
            pltpu.VMEM((nodes, feat), BF),
            pltpu.VMEM((2, chunks, UNITS, feat), BF),
            pltpu.VMEM((2, chunks, UNITS, classes), BF),
            pltpu.SemaphoreType.DMA,
            pltpu.SemaphoreType.DMA((2,)),
            pltpu.SemaphoreType.DMA((2,)),
        ],
        compiler_params=params(32),
        cost_estimate=cost(10.7, 16, 0.0021),
        name="first",
    )(place, asked, in_hbm(features), in_hbm(w_in), in_hbm(w_out))
    hidden, w_out_o, logits, prior_near, tiles_near = pl.pallas_call(
        second_kernel,
        grid=(steps,),
        in_specs=[smem, vmem, hbm, hbm, hbm, hbm, hbm, hbm, hbm],
        out_specs=[vmem] * 5,
        out_shape=[
            pltpu.VMEM((hid, rows), BF),
            pltpu.VMEM((128, UNITS, classes), BF),
            pltpu.VMEM((rows, classes), F32),
            pltpu.VMEM((nodes, classes), BF),
            pltpu.VMEM(tile_weights.shape, BF),
        ],
        scratch_shapes=[
            pltpu.VMEM((classes, rows), F32),
            pltpu.VMEM((2, chunks, UNITS, feat), BF),
            pltpu.SemaphoreType.DMA((2,)),
            pltpu.SemaphoreType.DMA((8,)),
            pltpu.SemaphoreType.DMA((4,)),
        ],
        compiler_params=params(16),
        cost_estimate=cost(6.5, 22, 0.0021),
        name="second",
    )(
        place,
        x,
        in_hbm(w_in),
        in_hbm(w_out),
        in_hbm(hidden_first),
        in_hbm(part),
        in_hbm(prior),
        in_hbm(tile_weights),
        halo,
    )

    row_tiles = tile_weights.shape[0]
    per = 2
    given = jnp.where(labeled == 1, label_class, -1).reshape(row_tiles, LANES)
    prop, residue, errors = pl.pallas_call(
        spread_kernel,
        grid=(row_tiles // per,),
        in_specs=[
            smem,
            vmem,
            vmem,
            vmem,
            once((halo_count // LANES, LANES)),
            once((row_tiles, LANES)),
            once((LANES, slots)),
            vmem,
        ],
        out_specs=[
            pl.BlockSpec((per * LANES, classes), lambda i: (i, 0)),
            vmem,
            whole((LANES, LANES)),
        ],
        out_shape=[
            jax.ShapeDtypeStruct((nodes, classes), BF),
            pltpu.VMEM((rows, classes), BF),
            jax.ShapeDtypeStruct((LANES, LANES), F32),
        ],
        scratch_shapes=[
            pltpu.VMEM((halo_count, classes), BF),
            pltpu.VMEM((nodes, classes), BF),
            pltpu.VMEM((rows, nodes), BF),
        ],
        compiler_params=params(22),
        cost_estimate=cost(4.3, 12, 0.0005),
        name="spread",
    )(tile_cols, tiles_near, prior_near, halo, hslot, given, asked, logits)

    partner = [(d, d ^ 1) for d in range(128)]
    part_rows = 2 * HBLK

    def peer_part(part):
        grad = pl.pallas_call(
            partial(peer_kernel, part),
            grid_spec=pltpu.PrefetchScalarGridSpec(
                num_scalar_prefetch=1,
                grid=(2,),
                in_specs=[
                    vmem,
                    vmem,
                    vmem,
                    vmem,
                ],
                out_specs=rows_at(0, classes + feat),
            ),
            out_shape=jax.ShapeDtypeStruct((part_rows, classes + feat), BF),
            compiler_params=params(22),
            cost_estimate=cost(4.3, 9),
        )(place, w_out_o, hidden, residue, x)
        return lax.ppermute(grad, DEV, partner)

    b_spec = pl.BlockSpec((1, 256, 512), lambda i, p: (i, 0, 0))
    c_spec = pl.BlockSpec((1, 4, 64, 512), lambda i, p: (i, 0, 0, 0))
    b_shape = pltpu.HBM((2, 256, 512), BF)
    c_shape = pltpu.HBM((2, 4, 64, 512), BF)

    def own_part(part, arrived):
        return pl.pallas_call(
            partial(own_kernel, part),
            grid_spec=pltpu.PrefetchScalarGridSpec(
                num_scalar_prefetch=1,
                grid=(2,),
                in_specs=[
                    vmem,
                    vmem,
                    vmem,
                    vmem,
                    rows_at(0, classes + feat),
                    once((LANES, LANES)),
                ],
                out_specs=[rows_at(0, classes), b_spec, b_spec, c_spec, c_spec, whole((LANES, LANES))],
            ),
            out_shape=[
                pltpu.HBM((part_rows, classes), BF),
                b_shape,
                b_shape,
                c_shape,
                c_shape,
                jax.ShapeDtypeStruct((LANES, LANES), F32),
            ],
            compiler_params=params(24),
            cost_estimate=cost(4.3, 12),
        )(place, w_out_o, hidden, residue, x, arrived, errors)

    arrived = [peer_part(0), peer_part(1)]
    *first, _ = own_part(0, arrived[0])
    *second, errors_out = own_part(1, arrived[1])
    grad_in, grad_out, row_error = summed_over_chips(first, second, halves, errors_out[:, :BATCH_SLOTS], bo, brank)
    return prop, row_error.reshape(batch), grad_in, grad_out


def solution(mesh):
    split = Mesh(mesh.devices.reshape(128), (DEV,))
    in_specs = (
        P(DEV, None),
        P(DEV),
        P(DEV),
        P(DEV, None),
        P(DEV, None),
        P(DEV, None, None, None),
        P(DEV, None),
        P(DEV),
        P(DEV, None),
        P(DEV),
        P(),
        P(),
    )
    out_specs = (P(DEV, None), P(DEV), P(DEV, None), P(DEV, None))
    return jax.shard_map(on_device, mesh=split, in_specs=in_specs, out_specs=out_specs, check_vma=False)
```

```python
from functools import partial

import jax
import jax.numpy as jnp
from jax import lax
from jax.experimental import pallas as pl
from jax.experimental.pallas import tpu as pltpu
from jax.sharding import Mesh
from jax.sharding import PartitionSpec as P


DEV = "dev"
BF = jnp.bfloat16
F32 = jnp.float32
LANES = 128
HALO_SLOTS = 4
BATCH_SLOTS = 8
UNITS = 32
HBLK = 512


def params(mib=48, **more):
    return pltpu.CompilerParams(vmem_limit_bytes=mib * 2**20, **more)


def cost(gigaflops, mib, gigaexp=0.0):
    return pl.CostEstimate(flops=int(gigaflops * 1e9), bytes_accessed=int(mib * 2**20), transcendentals=int(gigaexp * 1e9))


def in_hbm(x):
    return pltpu.with_memory_space_constraint(x, pltpu.HBM)


def dot(left, right, dims):
    return lax.dot_general(left, right, ((dims[:1], dims[1:]), ((), ())), preferred_element_type=F32)


def ranks_of(owner_ref, blocks):
    below = lax.broadcasted_iota(jnp.int32, (LANES, LANES), 0)
    along = lax.broadcasted_iota(jnp.int32, (LANES, LANES), 1)
    rows = [owner_ref[b : b + 1, :] for b in range(blocks)]
    cols = [jnp.broadcast_to(row, (LANES, LANES)).T for row in rows]
    ranks = []
    for i in range(blocks):
        earlier = jnp.zeros((LANES, LANES), F32)
        for j in range(i + 1):
            same = cols[j] == rows[i]
            if j == i:
                same = same & (below < along)
            earlier = earlier + same.astype(F32)
        ranks.append(jnp.sum(earlier, axis=0, keepdims=True).astype(jnp.int32))
    return rows, ranks


def request_kernel(ho, hl, bo, bl, table, hslot, brank):
    device = lax.broadcasted_iota(jnp.int32, (LANES, LANES), 0)
    lane = lax.broadcasted_iota(jnp.int32, (LANES, LANES), 1)
    out = jnp.zeros((LANES, LANES), F32)
    at = 0
    for owner, local, count in ((ho, hl, HALO_SLOTS), (bo, bl, BATCH_SLOTS)):
        blocks = owner.shape[0]
        rows, ranks = ranks_of(owner, blocks)
        for s in range(count):
            total = jnp.zeros((LANES, LANES), F32)
            for i in range(blocks):
                hit = (device == rows[i]) & (ranks[i] == s)
                named = (local[i : i + 1, :] + 1).astype(F32)
                total = total + jnp.where(hit, jnp.broadcast_to(named, (LANES, LANES)), 0.0)
            out = jnp.where(lane == at, jnp.sum(total, axis=1, keepdims=True), out)
            at += 1
        for i in range(blocks):
            if owner is ho:
                hslot[i : i + 1, :] = rows[i] * HALO_SLOTS + ranks[i]
            else:
                brank[i : i + 1, :] = ranks[i]
    table[...] = out.astype(jnp.int32) - 1


def returned_kernel(errors, bo, brank, out):
    device = lax.broadcasted_iota(jnp.int32, (LANES, LANES), 0)
    for i in range(bo.shape[0]):
        total = jnp.zeros((LANES, LANES), F32)
        for s in range(BATCH_SLOTS):
            hit = (device == bo[i : i + 1, :]) & (brank[i : i + 1, :] == s)
            total = total + jnp.where(hit, errors[:, s : s + 1], 0.0)
        out[i : i + 1, :] = jnp.sum(total, axis=0, keepdims=True)


def pick_rows(table, first, count, nodes, onehot):
    node = lax.broadcasted_iota(jnp.int32, (LANES, nodes), 1)
    for s in range(count):
        wanted = table[:, first + s : first + s + 1]
        onehot[s * LANES : (s + 1) * LANES, :] = (node == wanted).astype(F32).astype(BF)


def weight_chunks(core, block):
    half = block // 4
    holder = jnp.where(half == 1, core, 1 - core)
    turn = 1 - holder
    a = (block % 4 + turn) % 4
    sources = []
    for n in range(HBLK // UNITS):
        b = (n // 4 + turn) % 4
        c = (n % 4 + turn) % 4
        sources.append(((a * 4 + b) * 4 + c) * 2 + holder)
    return sources


def fetch_chunks(core, block, far, near, sem):
    for n, source in enumerate(weight_chunks(core, block)):
        pltpu.make_async_copy(far.at[source], near.at[n], sem).start()


def first_kernel(place, table, features, w_in, x, hidden, onehot, nodes_x, in_buf, nodes_sem, in_sem):
    step = pl.program_id(0)
    steps = pl.num_programs(0)
    chunks = HBLK // UNITS
    core = place[3]

    def fetch(block, slot):
        fetch_chunks(core, block, w_in, in_buf.at[slot], in_sem.at[slot])

    @pl.when(step == 0)
    def _():
        whole = pltpu.make_async_copy(features, nodes_x, nodes_sem)
        whole.start()
        fetch(0, 0)
        pick_rows(table, HALO_SLOTS, BATCH_SLOTS, features.shape[0], onehot)
        whole.wait()
        x[...] = dot(onehot[...], nodes_x[...], (1, 0)).astype(BF)

    slot = step % 2

    @pl.when(step + 1 < steps)
    def _():
        fetch(step + 1, 1 - slot)

    pltpu.make_async_copy(w_in.at[pl.ds(0, chunks)], in_buf.at[slot], in_sem.at[slot]).wait()
    h = jnp.tanh(dot(in_buf[slot].reshape(HBLK, in_buf.shape[3]), x[...], (1, 1))).astype(BF)
    hidden[...] = h


def second_kernel(
    place, x, w_in, w_out, hidden_far, prior_far, tiles_far, halo,
    hidden, w_out_near, logits, prior, tiles,
    acc, in_buf, in_sem, out_sem, sems,
):
    step = pl.program_id(0)
    steps = pl.num_programs(0)
    chunks = HBLK // UNITS
    core = place[3]
    done = hidden_far.shape[0]
    pairs = ((hidden_far, hidden.at[pl.ds(0, done)]), (prior_far, prior), (tiles_far, tiles))
    copies = [pltpu.make_async_copy(far, near, sems.at[n]) for n, (far, near) in enumerate(pairs)]

    def fetch(block, slot):
        fetch_chunks(core, block, w_in, in_buf.at[slot], in_sem.at[slot])

    def fetch_out(block):
        for n, source in enumerate(weight_chunks(core, block)):
            pltpu.make_async_copy(w_out.at[source], w_out_near.at[block * chunks + n], out_sem.at[block]).start()

    @pl.when(step == 0)
    def _():
        fetch(steps, 0)
        fetch_out(steps)
        acc[...] = jnp.zeros(acc.shape, F32)

    slot = step % 2

    @pl.when(step + 1 < steps)
    def _():
        fetch(steps + step + 1, 1 - slot)
        fetch_out(steps + step + 1)

    @pl.when(step == 0)
    def _():
        for copy in copies:
            copy.start()
        for block in range(4):
            fetch_out(block)

    def out_wait(block):
        here = w_out_near.at[pl.ds(block * chunks, chunks)]
        pltpu.make_async_copy(w_out.at[pl.ds(0, chunks)], here, out_sem.at[block]).wait()

    pltpu.make_async_copy(w_in.at[pl.ds(0, chunks)], in_buf.at[slot], in_sem.at[slot]).wait()
    out_wait(steps + step)
    h = jnp.tanh(dot(in_buf[slot].reshape(HBLK, in_buf.shape[3]), x[...], (1, 1))).astype(BF)
    hidden[pl.ds(pl.multiple_of(done + step * HBLK, HBLK), HBLK), :] = h
    w_out_here = w_out_near[pl.ds((steps + step) * chunks, chunks)].reshape(HBLK, w_out_near.shape[2])
    acc[...] += dot(w_out_here, h, (0, 0))

    @pl.when(step == steps - 2)
    def _():
        copies[0].wait()

    @pl.when(step >= steps - 2)
    def _():
        pair = 2 * (step - (steps - 2))
        out_wait(pair)
        out_wait(pair + 1)
        early = w_out_near[pl.ds(pair * chunks, 2 * chunks)].reshape(2 * HBLK, w_out_near.shape[2])
        acc[...] += dot(early, hidden[pl.ds(pl.multiple_of(pair * HBLK, HBLK), 2 * HBLK), :], (0, 0))

    @pl.when(step == steps - 1)
    def _():
        logits[...] = acc[...].T
        for copy in copies[1:]:
            copy.wait()


def spread_kernel(
    cols, weights, prior, halo, hslot, given, table, logits, prop, residue, errors, halo_tab, prop_all, onehot
):
    step = pl.program_id(0)
    per = weights.shape[0] // pl.num_programs(0)
    classes = prior.shape[1]

    @pl.when(step == 0)
    def _():
        owner = lax.broadcasted_iota(jnp.int32, (LANES, LANES), 0) * HALO_SLOTS
        for b in range(2):
            near = jnp.zeros((LANES, classes), F32)
            for k in range(HALO_SLOTS):
                pick = (owner + k == hslot[b : b + 1, :]).astype(F32).astype(BF)
                near = near + dot(pick, halo[:, k, :], (0, 0))
            halo_tab[b * LANES : (b + 1) * LANES, :] = near.astype(BF)

    for t in range(per):
        r = step * per + t
        acc = jnp.zeros((LANES, classes), F32)
        wide = jnp.zeros((LANES, LANES), F32)
        for m in range(4):
            pair = []
            for k in (2 * m, 2 * m + 1):
                wide = wide + weights[r, k].astype(F32)
                c = cols[r, k]
                if k < 6:
                    pair.append(prior[pl.ds(pl.multiple_of(c * LANES, LANES), LANES), :])
                else:
                    pair.append(halo_tab[pl.ds(pl.multiple_of((c - 16) * LANES, LANES), LANES), :])
            left = jnp.concatenate([weights[r, 2 * m], weights[r, 2 * m + 1]], axis=1)
            acc = acc + dot(left, jnp.concatenate(pair, axis=0), (1, 0))
        degree = jnp.sum(wide, axis=1, keepdims=True)
        mark = jnp.broadcast_to(given[pl.ds(r, 1), :], (LANES, LANES)).T
        lane = lax.broadcasted_iota(jnp.int32, (LANES, LANES), 1)
        seeds = jnp.concatenate([(mark == lane + g * LANES).astype(F32) for g in range(classes // LANES)], axis=1)
        mixed = (0.8 * (acc / degree) + 0.2 * seeds).astype(BF)
        prop[t * LANES : (t + 1) * LANES, :] = mixed
        prop_all[pl.ds(pl.multiple_of(r * LANES, LANES), LANES), :] = mixed

    @pl.when(step == pl.num_programs(0) - 1)
    def _():
        pick_rows(table, HALO_SLOTS, BATCH_SLOTS, prop_all.shape[0], onehot)
        lane = lax.broadcasted_iota(jnp.int32, (LANES, LANES), 1)
        out = jnp.zeros((LANES, LANES), F32)
        tall = 512
        for s in range(BATCH_SLOTS):
            at = slice(s * LANES, (s + 1) * LANES)
            if s % 4 == 0:
                picked = dot(onehot[s * LANES : s * LANES + tall, :], prop_all[...], (1, 0))
            log_z = jnp.log(picked[s % 4 * LANES : (s % 4 + 1) * LANES])
            target = log_z - jnp.mean(log_z, axis=1, keepdims=True)
            valid = table[:, HALO_SLOTS + s : HALO_SLOTS + s + 1] >= 0
            differ = jnp.where(valid, logits[at, :] - target, 0.0)
            out = jnp.where(lane == s, 0.5 * jnp.mean(differ * differ, axis=1, keepdims=True), out)
            residue[at, :] = (differ * (1.0 / 256.0)).astype(BF)
        errors[...] = out


def gradients(block, w_out, hidden, residue, x):
    at = pl.ds(pl.multiple_of(block * HBLK, HBLK), HBLK)
    h = hidden[at, :]
    wide = h.astype(F32)
    chunks = HBLK // UNITS
    w_out_here = w_out[pl.ds(block * chunks, chunks)].reshape(HBLK, w_out.shape[2])
    back = (dot(w_out_here, residue[...], (1, 1)) * (1.0 - wide * wide)).astype(BF)
    return dot(h, residue[...], (1, 0)), dot(back, x[...], (1, 0))


def peer_kernel(part, place, w_out, hidden, residue, x, grad):
    half = place[4] if part else 1 - place[4]
    out, into = gradients(2 * half + pl.program_id(0), w_out, hidden, residue, x)
    grad[:, :512] = out.astype(BF)
    grad[:, 512:] = into.astype(BF)


def own_kernel(part, place, w_out, hidden, residue, x, arrived, errors, a, send_b, keep_b, send_c, keep_c, errors_to):
    half = place[0] if part else 1 - place[0]
    out, into = gradients(4 + 2 * half + pl.program_id(0), w_out, hidden, residue, x)
    a[...] = (out + arrived[:, :512].astype(F32)).astype(BF)
    total = (into + arrived[:, 512:].astype(F32)).astype(BF)
    left = total[:, :512].reshape(2, 256, 512)
    right = total[:, 512:].reshape(4, 2, 64, 512)

    for half in range(2):

        @pl.when(place[1] == half)
        def _():
            keep_b[0] = left[half]
            send_b[0] = left[1 - half]

        @pl.when(place[2] == half)
        def _():
            keep_c[0] = right[:, half]
            send_c[0] = right[:, 1 - half]

    errors_to[...] = errors[...]


def pairing(level, dims):
    flip = 3 if level == 1 else 1
    pairs = []
    for source in range(128):
        core = source % 2
        spot = [source // 32, (source // 8) % 4, (source // 2) % 4]
        for d in dims:
            shifted = (spot[d] - (1 - core)) % 4
            spot[d] = ((shifted ^ flip) + (1 - core)) % 4
        pairs.append((source, ((spot[0] * 4 + spot[1]) * 4 + spot[2]) * 2 + core))
    return pairs


def exchange(x, level, dims):
    return lax.ppermute(x, DEV, pairing(level, dims))


def corners():
    groups = []
    for core in range(2):
        for high in range(8):
            group = []
            for low in range(8):
                shifted = [2 * ((high >> (2 - d)) & 1) + ((low >> (2 - d)) & 1) for d in range(3)]
                a, b, c = ((v + 1 - core) % 4 for v in shifted)
                group.append(((a * 4 + b) * 4 + c) * 2 + core)
            groups.append(group)
    return groups


def deal_kernel(k0, r0, k1, r1, k2, r2, pieces):
    for m in range(8):
        at = (m >> 2, (m >> 1) & 1, m & 1)
        for j, (k, r) in enumerate(((k0, r0), (k1, r1), (k2, r2))):
            piece = k[at].astype(F32) + r[at].astype(F32)
            pieces[m, :, j * 512 : (j + 1) * 512] = piece.astype(BF)


def finish_kernel(dealt, into, out):
    total = jnp.sum(dealt[...].astype(F32), axis=0)
    out[...] = total[:, :512]
    into[...] = total[:, 512:]


def summed_over_chips(first, second, halves):
    shape_a, shape_b, shape_c = (2, 4, 4, UNITS, 512), (2, 2, 4, UNITS, 512), (2, 4, 2, UNITS, 512)
    send_a, send_b1, keep_b1, send_c1, keep_c1 = first
    keep_a, send_b2, keep_b2, send_c2, keep_c2 = second
    got_c1 = exchange(send_c1, 1, (2,)).reshape(shape_c)
    got_b1 = exchange(send_b1, 1, (1,)).reshape(shape_b)
    got_a = exchange(send_a, 1, (0,)).reshape(shape_a)
    got_c2 = exchange(send_c2, 1, (2,)).reshape(shape_c)
    got_b2 = exchange(send_b2, 1, (1,)).reshape(shape_b)
    keep_a = keep_a.reshape(shape_a)
    keep_b1, keep_b2 = keep_b1.reshape(shape_b), keep_b2.reshape(shape_b)
    keep_c1, keep_c2 = keep_c1.reshape(shape_c), keep_c2.reshape(shape_c)

    def added(kept, got, dim=None, half=None):
        if dim is not None:
            kept, got = (lax.dynamic_slice_in_dim(v, 2 * half, 2, dim) for v in (kept, got))
        return kept.astype(F32) + got.astype(F32)

    def sent(value, dim):
        return exchange(value.astype(BF), 1, (dim,))

    _, hb, hc = halves
    c1_send = added(keep_c1, got_c1, 1, 1 - hb)
    c1_got = sent(c1_send, 1)
    b_send = added(keep_b1, got_b1)
    b_got = sent(b_send, 0)
    a_send = added(keep_a, got_a, 2, 1 - hc)
    a_got = sent(a_send, 2)
    c2_send = added(keep_c2, got_c2, 1, 1 - hb).astype(BF)
    c2_got = sent(c2_send, 1)
    b = added(keep_b2, got_b2).astype(BF)
    a = added(keep_a, got_a, 2, hc).astype(BF)
    c1 = added(keep_c1, got_c1, 1, hb).astype(BF)
    c2 = added(keep_c2, got_c2, 1, hb).astype(BF)
    b_last = sent(added(b, b_got, 2, 1 - hc), 2)
    a_last = sent(added(a, a_got, 1, 1 - hb), 1)
    c_send = added(c1, c1_got).astype(BF)
    c_last = sent(c_send, 0)
    b = added(b, b_got, 2, hc)
    a = added(a, a_got, 1, hb)
    c = added(c2, c2_got)
    pieces = pl.pallas_call(
        deal_kernel,
        in_specs=[pl.BlockSpec(memory_space=pltpu.VMEM)] * 6,
        out_specs=pl.BlockSpec(memory_space=pltpu.VMEM),
        out_shape=jax.ShapeDtypeStruct((8, UNITS, 1536), BF),
        compiler_params=params(16),
        name="deal",
    )(a, a_last, b, b_last, c, c_last)
    dealt = lax.all_to_all(pieces, DEV, 0, 0, axis_index_groups=corners(), tiled=True)
    return pl.pallas_call(
        finish_kernel,
        in_specs=[pl.BlockSpec(memory_space=pltpu.VMEM)],
        out_shape=[jax.ShapeDtypeStruct((UNITS, 1024), F32), jax.ShapeDtypeStruct((UNITS, 512), F32)],
        name="finish",
    )(pltpu.with_memory_space_constraint(dealt, pltpu.VMEM))


def on_device(prior, label_class, labeled, features, tile_cols, tile_weights, halo_owner, halo_local, batch_owner, batch_local, w_in, w_out):
    nodes, classes = prior.shape
    feat = features.shape[1]
    hid = w_in.shape[0]
    halo_count = halo_local.shape[0]
    batch = batch_local.shape[0]
    rows = BATCH_SLOTS * LANES
    me = lax.axis_index(DEV)
    core = me % 2
    chip = (me // 32, (me // 8) % 4, (me // 2) % 4)
    spots = [(s + 3 + core) % 4 for s in chip]
    halves = [s // 2 for s in spots]
    peer_half = (chip[0] + 4 - core) % 4 // 2
    place = jnp.stack([*halves, core, peer_half]).astype(jnp.int32)
    vmem = pl.BlockSpec(memory_space=pltpu.VMEM)
    smem = pl.BlockSpec(memory_space=pltpu.SMEM)
    hbm = pl.BlockSpec(memory_space=pl.ANY)
    i32 = jnp.int32

    bo = batch_owner.reshape(batch // LANES, LANES)
    table, hslot, brank = pl.pallas_call(
        request_kernel,
        in_specs=[vmem] * 4,
        out_shape=[
            jax.ShapeDtypeStruct((LANES, LANES), i32),
            jax.ShapeDtypeStruct((halo_count // LANES, LANES), i32),
            jax.ShapeDtypeStruct((batch // LANES, LANES), i32),
        ],
        name="request",
    )(
        halo_owner.reshape(halo_count // LANES, LANES),
        halo_local.reshape(halo_count // LANES, LANES),
        bo,
        batch_local.reshape(batch // LANES, LANES),
    )
    asked = lax.all_to_all(table[:, : HALO_SLOTS + BATCH_SLOTS], DEV, 0, 0, tiled=True)

    served = prior[jnp.maximum(asked[:, :HALO_SLOTS], 0)]
    halo = lax.all_to_all(served, DEV, 0, 0, tiled=True)

    def whole(shape):
        return pl.BlockSpec(shape, lambda i, *_: (0,) * len(shape))

    def once(shape):
        return pl.BlockSpec(shape, lambda i, *_: (0,) * len(shape), pipeline_mode=pl.Buffered(1))

    def rows_at(offset, width):
        return pl.BlockSpec((HBLK, width), lambda i, *_: (i + offset, 0))

    slots = HALO_SLOTS + BATCH_SLOTS
    chunks = HBLK // UNITS
    steps = hid // HBLK // 2
    w_in = w_in.reshape(128, UNITS, feat)
    w_out = w_out.reshape(128, UNITS, classes)
    x, hidden_first = pl.pallas_call(
        first_kernel,
        grid=(steps,),
        in_specs=[smem, once((LANES, slots)), hbm, hbm],
        out_specs=[vmem, rows_at(0, rows)],
        out_shape=[pltpu.VMEM((rows, feat), BF), pltpu.HBM((hid // 2, rows), BF)],
        scratch_shapes=[
            pltpu.VMEM((rows, nodes), BF),
            pltpu.VMEM((nodes, feat), BF),
            pltpu.VMEM((2, chunks, UNITS, feat), BF),
            pltpu.SemaphoreType.DMA,
            pltpu.SemaphoreType.DMA((2,)),
        ],
        compiler_params=params(28),
        cost_estimate=cost(8.6, 14, 0.0021),
        name="first",
    )(place, asked, in_hbm(features), in_hbm(w_in))
    hidden, w_out_o, logits, prior_near, tiles_near = pl.pallas_call(
        second_kernel,
        grid=(steps,),
        in_specs=[smem, vmem, hbm, hbm, hbm, hbm, hbm, hbm],
        out_specs=[vmem] * 5,
        out_shape=[
            pltpu.VMEM((hid, rows), BF),
            pltpu.VMEM((128, UNITS, classes), BF),
            pltpu.VMEM((rows, classes), F32),
            pltpu.VMEM((nodes, classes), BF),
            pltpu.VMEM(tile_weights.shape, BF),
        ],
        scratch_shapes=[
            pltpu.VMEM((classes, rows), F32),
            pltpu.VMEM((2, chunks, UNITS, feat), BF),
            pltpu.SemaphoreType.DMA((2,)),
            pltpu.SemaphoreType.DMA((8,)),
            pltpu.SemaphoreType.DMA((3,)),
        ],
        compiler_params=params(16),
        cost_estimate=cost(8.6, 18, 0.0021),
        name="second",
    )(
        place,
        x,
        in_hbm(w_in),
        in_hbm(w_out),
        in_hbm(hidden_first),
        in_hbm(prior),
        in_hbm(tile_weights),
        halo,
    )

    row_tiles = tile_weights.shape[0]
    per = 2
    given = jnp.where(labeled == 1, label_class, -1).reshape(row_tiles, LANES)
    prop, residue, errors = pl.pallas_call(
        spread_kernel,
        grid=(row_tiles // per,),
        in_specs=[
            smem,
            vmem,
            vmem,
            vmem,
            once((halo_count // LANES, LANES)),
            once((row_tiles, LANES)),
            once((LANES, slots)),
            vmem,
        ],
        out_specs=[
            pl.BlockSpec((per * LANES, classes), lambda i: (i, 0)),
            vmem,
            whole((LANES, LANES)),
        ],
        out_shape=[
            jax.ShapeDtypeStruct((nodes, classes), BF),
            pltpu.VMEM((rows, classes), BF),
            jax.ShapeDtypeStruct((LANES, LANES), F32),
        ],
        scratch_shapes=[
            pltpu.VMEM((halo_count, classes), BF),
            pltpu.VMEM((nodes, classes), BF),
            pltpu.VMEM((rows, nodes), BF),
        ],
        compiler_params=params(22),
        cost_estimate=cost(4.3, 12, 0.0005),
        name="spread",
    )(tile_cols, tiles_near, prior_near, halo, hslot, given, asked, logits)

    partner = [(d, d ^ 1) for d in range(128)]
    part_rows = 2 * HBLK

    def peer_part(part):
        grad = pl.pallas_call(
            partial(peer_kernel, part),
            grid_spec=pltpu.PrefetchScalarGridSpec(
                num_scalar_prefetch=1,
                grid=(2,),
                in_specs=[
                    vmem,
                    vmem,
                    vmem,
                    vmem,
                ],
                out_specs=rows_at(0, classes + feat),
            ),
            out_shape=jax.ShapeDtypeStruct((part_rows, classes + feat), BF),
            compiler_params=params(22),
            cost_estimate=cost(4.3, 9),
        )(place, w_out_o, hidden, residue, x)
        return lax.ppermute(grad, DEV, partner)

    b_spec = pl.BlockSpec((1, 256, 512), lambda i, p: (i, 0, 0))
    c_spec = pl.BlockSpec((1, 4, 64, 512), lambda i, p: (i, 0, 0, 0))
    b_shape = pltpu.HBM((2, 256, 512), BF)
    c_shape = pltpu.HBM((2, 4, 64, 512), BF)

    def own_part(part, arrived):
        return pl.pallas_call(
            partial(own_kernel, part),
            grid_spec=pltpu.PrefetchScalarGridSpec(
                num_scalar_prefetch=1,
                grid=(2,),
                in_specs=[
                    vmem,
                    vmem,
                    vmem,
                    vmem,
                    rows_at(0, classes + feat),
                    once((LANES, LANES)),
                ],
                out_specs=[rows_at(0, classes), b_spec, b_spec, c_spec, c_spec, whole((LANES, LANES))],
            ),
            out_shape=[
                pltpu.HBM((part_rows, classes), BF),
                b_shape,
                b_shape,
                c_shape,
                c_shape,
                jax.ShapeDtypeStruct((LANES, LANES), F32),
            ],
            compiler_params=params(24),
            cost_estimate=cost(4.3, 12),
        )(place, w_out_o, hidden, residue, x, arrived, errors)

    arrived = [peer_part(0), peer_part(1)]
    *first, _ = own_part(0, arrived[0])
    *second, errors_out = own_part(1, arrived[1])
    grad_in, grad_out = summed_over_chips(first, second, halves)

    back_errors = lax.all_to_all(errors_out[:, :BATCH_SLOTS], DEV, 0, 0, tiled=True)
    row_error = pl.pallas_call(
        returned_kernel,
        in_specs=[vmem] * 3,
        out_shape=jax.ShapeDtypeStruct((batch // LANES, LANES), F32),
        name="returned",
    )(back_errors, bo, brank).reshape(batch)
    return prop, row_error, grad_in, grad_out


def solution(mesh):
    split = Mesh(mesh.devices.reshape(128), (DEV,))
    in_specs = (
        P(DEV, None),
        P(DEV),
        P(DEV),
        P(DEV, None),
        P(DEV, None),
        P(DEV, None, None, None),
        P(DEV, None),
        P(DEV),
        P(DEV, None),
        P(DEV),
        P(),
        P(),
    )
    out_specs = (P(DEV, None), P(DEV), P(DEV, None), P(DEV, None))
    return jax.shard_map(on_device, mesh=split, in_specs=in_specs, out_specs=out_specs, check_vma=False)
```
